128 devices in a mesh: seq: 32 (over z, y, core), opt: 4 (over x).
Axes of the slice: x: 4, y: 4, z: 4, core: 2. Of those that a mesh axis runs over, the one named last changes fastest.
Arguments:
- layer_in: bfloat16 [4, 16384, 4096], P('opt', 'seq'), may hold values from -48 to 48, as said below
- ssm_input: bfloat16 [4, 16384, 4096], P('opt', 'seq'), may hold values from -0.119628906 to 0.119628906
- grad_out: bfloat16 [4, 16384, 4096], P('opt', 'seq'), may hold values from -0.59765625 to 0.59765625
- log_decay: float32 [4, 32, 16384], P('opt', None, 'seq'), may hold values from -1 to 0, as said below
- skip_gain: float32 [32], replicated, may hold values from 0.5 to 2
- w_bc: float32 [4096, 256], P(('seq', 'opt')), may hold values from -0.0078125 to 0.0078125
- m_code: bfloat16 [4096, 256], P(('seq', 'opt')), may hold values from -1 to 1
- m_scale: float32 [256], replicated, may hold values from 0.0001 to 0.001
- row_stat: float32 [4096], P(('seq', 'opt')), may hold values from 3e-07 to 3e-06
- col_stat: float32 [256], replicated, may hold values from 3e-07 to 3e-06
Outputs:
- grad_input: bfloat16 [4, 16384, 4096], P('opt', 'seq')
- update: float32 [4096, 256], P(('seq', 'opt'))
- code_next: bfloat16 [4096, 256], P(('seq', 'opt'))
- scale_next: float32 [256], replicated
- row_next: float32 [4096], P(('seq', 'opt'))
- col_next: float32 [256], replicated
The draws below stay inside these ranges and needn't reach their ends.
Inputs may be any that keep to these rules, and one draw needn't show every extreme that they name: `layer_in`: real-valued rows of order one. `log_decay`: negative log decays.
All inputs are finite; a program needn't handle non-finite values.
Results may differ from the reference program's by a relative error of at most 0.0095.
Values may be sent and summed in bfloat16 or wider, within the bound.
A program may use at most 256 MiB of HBM per device.

```python
import math
import jax
import jax.numpy as jnp
from jax import lax

D = 4096
N = 128
P_SIZE = 128
H = 32
BLOCK = 256
TOK_DEV = 512
TOKEN_POSITIONS = 16384
SEQUENCE_COUNT = 4


def draw_layer_in(key, part):
    lookup_keys = jax.random.split(key, 2)
    position = jnp.arange(D, dtype=jnp.float32) / (D - 1)
    feature_scale = jnp.exp(math.log(3.0) * position + math.log(10.0) * jax.random.uniform(lookup_keys[0], (D,), jnp.float32)) / 4.0
    base = jnp.clip(jax.random.normal(lookup_keys[1], (SEQUENCE_COUNT, TOKEN_POSITIONS, D), jnp.float32), -6.0, 6.0)
    return (base * feature_scale[None, None, :]).astype(jnp.bfloat16)


def draw_log_decay(key, part):
    lookup_keys = jax.random.split(key, 7)
    share = 0.5
    fast_head = jax.random.uniform(lookup_keys[0], (SEQUENCE_COUNT, H, 1), jnp.float32) < share
    fast_rate = jax.random.uniform(lookup_keys[1], (SEQUENCE_COUNT, H, 1), jnp.float32, 1.0 / 50.0, 1.0 / 30.0)
    slow_rate = jax.random.uniform(lookup_keys[2], (SEQUENCE_COUNT, H, 1), jnp.float32, 0.2, 0.6) / TOKEN_POSITIONS
    rate = jnp.where(fast_head, fast_rate, slow_rate)
    rough = jnp.exp(jax.random.uniform(lookup_keys[3], (SEQUENCE_COUNT, H, TOKEN_POSITIONS), jnp.float32, -0.7, 0.7))
    blocks = TOKEN_POSITIONS // TOK_DEV
    device_factor = jnp.exp(jax.random.uniform(lookup_keys[4], (SEQUENCE_COUNT, H, blocks, 1), jnp.float32, -0.7, 0.7))
    device_factor = jnp.broadcast_to(device_factor, (SEQUENCE_COUNT, H, blocks, TOK_DEV)).reshape(SEQUENCE_COUNT, H, TOKEN_POSITIONS)
    first_spot = jax.random.randint(lookup_keys[5], (SEQUENCE_COUNT, 1, 1, 1), 0, TOKEN_POSITIONS)
    spot_offset = jax.random.randint(jax.random.fold_in(lookup_keys[5], 1), (SEQUENCE_COUNT, 1, 1, 1), 1, TOKEN_POSITIONS)
    second_spot = (first_spot + spot_offset) % TOKEN_POSITIONS
    flurry_position = jnp.concatenate([first_spot, second_spot], axis=-1).astype(jnp.int32)
    flurry_depth = jax.random.uniform(lookup_keys[6], (SEQUENCE_COUNT, 1, 1, 2), jnp.float32, 0.22, 0.69)
    target_spots = jnp.arange(TOKEN_POSITIONS, dtype=jnp.int32)[None, None, :, None]
    match_count = jnp.sum(jnp.where(target_spots == flurry_position, flurry_depth, 0.0), axis=-1)
    return -(rate * rough * device_factor) - match_count


def steps_of(stream_key, shape, pieces, smallest, top_value):
    level, own = 1.0, jax.random.fold_in(stream_key, 6)
    for dim, parts in pieces:
        draws = jnp.exp(jax.random.uniform(jax.random.fold_in(own, dim), (parts,), jnp.float32, smallest / len(pieces), top_value / len(pieces)))
        level = level * jnp.repeat(draws, shape[dim] // parts).reshape([-1 if axis == dim else 1 for axis in range(len(shape))])
    return level


def centred(rng, dims, scale, limit, shards=(), kind=jnp.bfloat16):
    drawn = jax.random.normal(rng, dims, jnp.float32) * scale
    if len(shards) > 0:
        drawn = steps_of(rng, dims, shards, -0.22, 0.18) * drawn
    return jnp.clip(drawn, min=-limit, max=limit).astype(kind)


def setup_inputs(seed: int = 0) -> dict:
    key_of = jax.random.split(jax.random.key(seed), 11)
    layer_in = draw_layer_in(jax.random.fold_in(key_of[10], 71), 0)
    ssm_input = centred(key_of[1], (SEQUENCE_COUNT, TOKEN_POSITIONS, H * P_SIZE), 0.02, 0.119628906, ((0, 4), (1, 32)))
    grad_out = centred(key_of[2], (SEQUENCE_COUNT, TOKEN_POSITIONS, H * P_SIZE), 0.1, 0.59765625, ((0, 4), (1, 32)))
    log_decay = draw_log_decay(jax.random.fold_in(key_of[10], 71), 0)
    skip_gain = jnp.clip(jax.random.uniform(key_of[4], (H,), jnp.float32, 0.5, 2.0), 0.5, 2.0)
    w_bc = centred(key_of[5], (D, 2 * N), (D * N) ** -0.5, 0.0078125, ((0, 128),), jnp.float32)
    m_code = jnp.clip(jax.random.uniform(key_of[6], (D, 2 * N), jnp.float32, -1.0, 1.0) * steps_of(key_of[6], (D, 2 * N), ((0, 128),), -0.4, 0.0), -1.0, 1.0).astype(jnp.bfloat16)
    m_scale = jnp.clip(jnp.exp(jax.random.uniform(key_of[7], (2 * N,), jnp.float32, math.log(0.0001), math.log(0.001))), 0.0001, 0.001)
    row_stat = jnp.clip(jnp.exp(math.log(3.000000106112566e-06) - 2.3025851 * jax.random.uniform(key_of[8], (D,), jnp.float32) ** steps_of(key_of[8], (D,), ((0, 128),), -0.2, 0.2)), 3.000000106112566e-07, 3.000000106112566e-06)
    col_stat = jnp.clip(jnp.exp(jax.random.uniform(key_of[9], (2 * N,), jnp.float32, math.log(3.000000106112566e-07), math.log(3.000000106112566e-06))), 3.000000106112566e-07, 3.000000106112566e-06)
    return {"layer_in": layer_in, "ssm_input": ssm_input, "grad_out": grad_out, "log_decay": log_decay, "skip_gain": skip_gain, "w_bc": w_bc, "m_code": m_code, "m_scale": m_scale, "row_stat": row_stat, "col_stat": col_stat}


beta_one = 0.9
beta_two = 0.95
weight_decay = 0.1
clip_norm = 1.0
tiny_square = 1e-30
adam_floor = 1e-08
peak_floor = 1e-06
norm_floor = 1e-06
highest = lax.Precision.HIGHEST

def lower_decays(running):
    length = running.shape[1]
    row_pos = lax.broadcasted_iota(jnp.int32, (length, length), 0)
    col_pos = lax.broadcasted_iota(jnp.int32, (length, length), 1)
    spread = running[:, :, None] - running[:, None, :]
    return jnp.exp(jnp.where((row_pos >= col_pos)[None], spread, -jnp.inf))

def state_adds(feat_blk, cot_blk, b_rows, c_rows, running):
    closing = running[:, -1]
    shrink = jnp.exp(closing[:, None] - running)
    grow = jnp.exp(running)
    forward_add = jnp.einsum('htn,thp->hnp', shrink[:, :, None] * b_rows[None], feat_blk, precision=highest)
    backward_add = jnp.einsum('htn,thp->hnp', grow[:, :, None] * c_rows[None], cot_blk, precision=highest)
    return (forward_add, backward_add)

def block_terms(feat_blk, cot_blk, b_rows, c_rows, running, state_in, grad_in, skip_gain):
    closing = running[:, -1]
    decays = lower_decays(running)
    grow = jnp.exp(running)
    shrink = jnp.exp(closing[:, None] - running)
    intersection = jnp.einsum('thp,shp->hts', feat_blk, cot_blk, precision=highest)
    affinity = jnp.dot(b_rows, c_rows.T, precision=highest)
    mixing = lax.optimization_barrier(jnp.sum(decays * jnp.transpose(intersection, (0, 2, 1)), axis=0))
    left_in = jnp.einsum('hnp,thp->htn', state_in, cot_blk, precision=highest)
    grad_cmat = jnp.dot(mixing, b_rows, precision=highest) + lax.optimization_barrier(jnp.sum(grow[:, :, None] * left_in, axis=0))
    right_in = jnp.einsum('hnp,thp->htn', grad_in, feat_blk, precision=highest)
    grad_bmat = jnp.dot(mixing.T, c_rows, precision=highest) + lax.optimization_barrier(jnp.sum(shrink[:, :, None] * right_in, axis=0))
    weighted = jnp.transpose(decays, (0, 2, 1)) * affinity[None]
    inner = jnp.einsum('hts,shp->thp', weighted, cot_blk, precision=highest)
    outer = jnp.einsum('tn,hnp->thp', b_rows, grad_in, precision=highest) * shrink.T[:, :, None]
    grad_feat = inner + outer + skip_gain[None, :, None] * cot_blk
    return (grad_feat, jnp.concatenate([grad_bmat, grad_cmat], axis=1))

def one_sequence(layer_rows, feat_rows, cot_rows, log_rows, w_half, skip_gain):
    proj = jnp.dot(layer_rows, w_half, preferred_element_type=jnp.float32).astype(jnp.bfloat16)
    count = TOKEN_POSITIONS // BLOCK
    b_all = proj[:, :N].astype(jnp.float32).reshape(count, BLOCK, N)
    c_all = proj[:, N:].astype(jnp.float32).reshape(count, BLOCK, N)
    feats = feat_rows.astype(jnp.float32).reshape(count, BLOCK, H, P_SIZE)
    cots = cot_rows.astype(jnp.float32).reshape(count, BLOCK, H, P_SIZE)
    logs = jnp.transpose(log_rows.reshape(H, count, BLOCK), (1, 0, 2))

    def forward(state, items):
        feat_blk, cot_blk, b_rows, c_rows, log_blk = items
        running = jnp.cumsum(log_blk, axis=1)
        forward_add, unused = state_adds(feat_blk, cot_blk, b_rows, c_rows, running)
        return (jnp.exp(running[:, -1])[:, None, None] * state + forward_add, state)
    start = jnp.zeros((H, N, P_SIZE), jnp.float32)
    unused_last, states_in = lax.scan(forward, start, (feats, cots, b_all, c_all, logs))

    def backward(grad_in, items):
        feat_blk, cot_blk, b_rows, c_rows, log_blk, state_in = items
        running = jnp.cumsum(log_blk, axis=1)
        grad_feat, grad_bc = block_terms(feat_blk, cot_blk, b_rows, c_rows, running, state_in, grad_in, skip_gain)
        unused, backward_add = state_adds(feat_blk, cot_blk, b_rows, c_rows, running)
        return (jnp.exp(running[:, -1])[:, None, None] * grad_in + backward_add, (grad_feat, grad_bc))
    unused_first, outputs = lax.scan(backward, start, (feats, cots, b_all, c_all, logs, states_in), reverse=True)
    grad_feats, grad_bcs = outputs
    grad_bc = grad_bcs.reshape(TOKEN_POSITIONS, 2 * N).astype(jnp.bfloat16)
    weight_grad = jnp.dot(layer_rows.T, grad_bc, preferred_element_type=jnp.float32)
    return (grad_feats.reshape(TOKEN_POSITIONS, H * P_SIZE).astype(jnp.bfloat16), weight_grad)

def reference(layer_in, ssm_input, grad_out, log_decay, skip_gain, w_bc, m_code, m_scale, row_stat, col_stat):
    w_half = w_bc.astype(jnp.bfloat16)
    results = []
    grad_sum = jnp.zeros((D, 2 * N), jnp.float32)
    for seq_id in range(SEQUENCE_COUNT):
        grad_feat, weight_grad = one_sequence(layer_in[seq_id], ssm_input[seq_id], grad_out[seq_id], log_decay[seq_id], w_half, skip_gain)
        results.append(grad_feat)
        grad_sum = grad_sum + weight_grad
    grad_input = jnp.stack(results)
    norm_sq = jnp.sum(grad_sum * grad_sum) + norm_floor
    factor = jnp.minimum(1.0, clip_norm / jnp.sqrt(norm_sq))
    scaled = grad_sum * factor
    squares = scaled * scaled
    moment = beta_one * m_code.astype(jnp.float32) * m_scale[None, :] + (1.0 - beta_one) * scaled
    row_next = beta_two * row_stat + (1.0 - beta_two) * (lax.optimization_barrier(jnp.mean(squares, axis=1)) + tiny_square)
    col_next = beta_two * col_stat + (1.0 - beta_two) * (lax.optimization_barrier(jnp.mean(squares, axis=0)) + tiny_square)
    second = row_next[:, None] * col_next[None, :] / jnp.mean(row_next)
    update = moment / (jnp.sqrt(second) + adam_floor) + weight_decay * w_bc
    scale_next = lax.optimization_barrier(jnp.max(jnp.abs(moment), axis=0)) + peak_floor
    code_next = (moment / scale_next[None, :]).astype(jnp.bfloat16)
    return (grad_input, update, code_next, scale_next, row_next, col_next)
```

```python
import functools

import jax
import jax.numpy as jnp
from jax import lax
from jax.experimental import pallas as pl
from jax.experimental.pallas import tpu as pltpu
from jax.sharding import PartitionSpec as P

MESH = pl.DeviceIdType.MESH
BLOCK = 256
N = 128
F32 = jnp.float32
BF16 = jnp.bfloat16
HIGH = lax.Precision.HIGHEST

beta_one = 0.9
beta_two = 0.95
weight_decay = 0.1
clip_norm = 1.0
tiny_square = 1e-30
adam_floor = 1e-08
peak_floor = 1e-06
norm_floor = 1e-06


def dot_nn(a, b, precision=None):
    return lax.dot_general(a, b, (((1,), (0,)), ((), ())), preferred_element_type=F32, precision=precision)


def dot_nt(a, b, precision=None):
    return lax.dot_general(a, b, (((1,), (1,)), ((), ())), preferred_element_type=F32, precision=precision)


def kernel(
    seqs,
    opts,
    x_hbm,
    dy_hbm,
    lay_hbm,
    logs_ref,
    skip_ref,
    w_ref,
    code_ref,
    mscale_ref,
    rowstat_ref,
    colstat_ref,
    gi_hbm,
    upd_ref,
    codeo_ref,
    scaleo_ref,
    rowo_ref,
    colo_ref,
    x_v,
    dy_v,
    lay_v,
    xs_v,
    ds_v,
    gi_v,
    w_v,
    logp_v,
    r_v,
    rt_v,
    erow_v,
    mix_v,
    aff_v,
    bc_v,
    bct_v,
    f0_v,
    k1_v,
    t_v,
    pt_v,
    cb_v,
    rb_v,
    ob_v,
    ib_v,
    xb_v,
    fin_v,
    gbt_v,
    wg_v,
    rd_v,
    rss_v,
    rsr_v,
    xo_v,
    xr_v,
    dlo_v,
    dlp_v,
    dc_v,
    a1s_v,
    a1r_v,
    a2s_v,
    a2r_v,
    m1s_v,
    m1r_v,
    m2s_v,
    m2r_v,
    in_sem,
    out_sem,
    send_sem,
    recv_sem,
    blk_sem,
    chunk_sem,
):
    heads = skip_ref.shape[0]
    chips = seqs // 2
    rows = w_ref.shape[0]
    rblk = rows * opts
    width = x_hbm.shape[1]
    dim = lay_hbm.shape[1]
    groups = 4
    per = chips // groups
    lanes_g = width // groups

    seq = lax.axis_index("seq")
    opt = lax.axis_index("opt")
    chip = seq // 2
    core = seq % 2
    mate = chip * 2 + (1 - core)
    partner = (mate, opt)

    def yz(k):
        other = (chip + k) % chips
        return other, (other * 2 + core, opt)

    def xp(k):
        other = (opt + k) % opts
        return other, (seq, other)

    def remote(src, dst, s_sem, r_sem, dev):
        return pltpu.make_async_remote_copy(
            src_ref=src, dst_ref=dst, send_sem=s_sem, recv_sem=r_sem, device_id=dev, device_id_type=MESH
        )

    def wait_bytes(ref, sem):
        pltpu.make_async_copy(ref, ref, sem).wait()

    def in_copies(g):
        lanes = pl.ds(g * lanes_g, lanes_g)
        return (
            pltpu.make_async_copy(x_hbm.at[:, lanes], x_v.at[:, lanes], in_sem.at[2 * g]),
            pltpu.make_async_copy(dy_hbm.at[:, lanes], dy_v.at[:, lanes], in_sem.at[2 * g + 1]),
        )

    lay_copy = pltpu.make_async_copy(lay_hbm, lay_v, in_sem.at[2 * groups])

    barrier = pltpu.get_barrier_semaphore()
    pl.semaphore_signal(barrier, inc=1, device_id=partner, device_id_type=MESH)
    for k in range(1, opts):
        other = (opt + k) % opts
        pl.semaphore_signal(barrier, inc=1, device_id=(seq, other), device_id_type=MESH)
        pl.semaphore_signal(barrier, inc=1, device_id=(mate, other), device_id_type=MESH)
    for k in range(1, chips):
        pl.semaphore_signal(barrier, inc=1, device_id=yz(k)[1], device_id_type=MESH)

    for g in range(groups):
        for copy in in_copies(g):
            copy.start()
    lay_copy.start()

    my_block = pl.multiple_of((chip * 2 + core) * rblk, rblk)
    my_rows = pl.multiple_of(my_block + opt * rows, rows)
    w_v[pl.ds(my_rows, rows), :] = w_ref[...].astype(BF16)

    logp_v[...] = jnp.zeros_like(logp_v)
    logp_v[0:heads, :] = logs_ref[...]
    row_i = lax.broadcasted_iota(jnp.int32, (BLOCK, BLOCK), 0)
    col_i = lax.broadcasted_iota(jnp.int32, (BLOCK, BLOCK), 1)
    upper = jnp.where(row_i <= col_i, 1.0, 0.0).astype(F32)
    lower = jnp.where(row_i >= col_i, 1.0, 0.0).astype(F32)
    for b in range(2):
        part = logp_v[:, b * BLOCK : (b + 1) * BLOCK]
        r_v[b] = dot_nn(part, upper, HIGH)
        rt_v[b * BLOCK : (b + 1) * BLOCK, :] = dot_nt(lower, part, HIGH)
    total = rt_v[BLOCK - 1 : BLOCK, :] + rt_v[2 * BLOCK - 1 : 2 * BLOCK, :]
    dlo_v[...] = jnp.broadcast_to(total, dlo_v.shape)

    pl.semaphore_wait(barrier, 1 + 2 * (opts - 1) + chips - 1)

    def w_rows(start, size):
        return w_v.at[pl.ds(start, size), :]

    for k in range(1, opts):
        remote(w_rows(my_rows, rows), w_rows(my_rows, rows), send_sem.at[0], recv_sem.at[0], xp(k)[1]).start()
    remote(dlo_v, dlp_v, send_sem.at[1], recv_sem.at[1], partner).start()

    mix_v[...] = jnp.zeros_like(mix_v)
    lane_i = lax.broadcasted_iota(jnp.int32, (2 * BLOCK, N), 1)

    def column(h):
        return jnp.sum(jnp.where(lane_i == h, rt_v[...], 0.0), axis=1, keepdims=True)

    half = BLOCK // 2
    tri_a = lax.broadcasted_iota(jnp.int32, (half, BLOCK), 1) >= lax.broadcasted_iota(jnp.int32, (half, BLOCK), 0)
    tri_b = lax.broadcasted_iota(jnp.int32, (half, half), 1) >= lax.broadcasted_iota(jnp.int32, (half, half), 0)

    def decays(rt, rs):
        top = jnp.exp(jnp.where(tri_a, rs - rt[0:half], -jnp.inf))
        bottom = jnp.exp(jnp.where(tri_b, rs[:, half:] - rt[half:], -jnp.inf))
        return top, bottom

    def mix_pair(hp, carry):
        adds = [[None, None], [None, None]]
        for j in range(2):
            h = hp * 2 + j
            lanes = pl.ds(pl.multiple_of(h * N, N), N)
            col = column(h)
            for b in range(2):
                at = pl.ds(b * BLOCK, BLOCK)
                xb = x_v[at, lanes]
                db = dy_v[at, lanes]
                rt = col[b * BLOCK : (b + 1) * BLOCK]
                rs = r_v[b, pl.ds(h, 1), :]
                prod = dot_nt(xb, db)
                top, bottom = decays(rt, rs)
                top = top * prod[0:half]
                bottom = bottom * prod[half:, half:]
                adds[b][0] = top if j == 0 else adds[b][0] + top
                adds[b][1] = bottom if j == 0 else adds[b][1] + bottom
                closing = rt[BLOCK - 1 : BLOCK]
                erow_v[b, :, lanes] = jnp.broadcast_to(jnp.exp(closing), (8, N))
                xs_v[at, lanes] = (xb.astype(F32) * jnp.exp(closing - rt)).astype(BF16)
                ds_v[at, lanes] = (db.astype(F32) * jnp.exp(rt)).astype(BF16)
        for b in range(2):
            mix_v[b, 0:half, :] += adds[b][0]
            mix_v[b, half:, half:] += adds[b][1]
        return carry

    pairs_g = heads // 2 // groups
    for g in range(groups):
        for copy in in_copies(g):
            copy.wait()
        lax.fori_loop(g * pairs_g, (g + 1) * pairs_g, mix_pair, 0)
        if g == 0:
            wait_bytes(w_rows(0, rows * (opts - 1)), recv_sem.at[0])
            for k in range(1, chips):
                remote(
                    w_rows(my_block, rblk), w_rows(my_block, rblk), send_sem.at[2], blk_sem.at[k], yz(k)[1]
                ).start()
            remote(w_rows(my_block, rblk), w_rows(my_block, rblk), send_sem.at[3], recv_sem.at[3], partner).start()
            wait_bytes(dlp_v, recv_sem.at[1])
            dc_v[chip] = dlo_v[...] + dlp_v[...]
            for k in range(1, chips):
                remote(dc_v.at[chip], dc_v.at[chip], send_sem.at[4], recv_sem.at[4], yz(k)[1]).start()

    for k in range(1, chips):
        source = (chip + chips - k) % chips
        start = pl.multiple_of((source * 2 + core) * rblk, rblk)
        wait_bytes(w_rows(start, rblk), blk_sem.at[k])
        remote(w_rows(start, rblk), w_rows(start, rblk), send_sem.at[3], recv_sem.at[3], partner).start()
    lay_copy.wait()
    wait_bytes(w_rows(0, rblk * chips), recv_sem.at[3])

    proj = dot_nn(lay_v[...], w_v[...]).astype(BF16)
    bc_v[...] = proj
    bct_v[...] = jnp.transpose(proj.astype(F32)).astype(BF16)
    for b in range(2):
        at = slice(b * BLOCK, (b + 1) * BLOCK)
        aff_v[b] = dot_nt(bc_v[at, 0:N], bc_v[at, N : 2 * N])

    def add_pair(o, carry):
        lanes = pl.ds(pl.multiple_of(o * 2 * N, 2 * N), 2 * N)
        e0 = erow_v[0, 0:1, lanes]
        e1 = erow_v[1, 0:1, lanes]
        f0 = dot_nn(bct_v[0:N, 0:BLOCK], xs_v[0:BLOCK, lanes])
        f1 = dot_nn(bct_v[0:N, BLOCK:], xs_v[BLOCK:, lanes])
        k0 = dot_nn(bct_v[N:, 0:BLOCK], ds_v[0:BLOCK, lanes])
        k1 = dot_nn(bct_v[N:, BLOCK:], ds_v[BLOCK:, lanes])
        f0_v[:, lanes] = f0
        k1_v[:, lanes] = k1
        state = (e1 * f0 + f1).astype(BF16)
        grad = (k0 + e0 * k1).astype(BF16)
        for j in range(2):
            t_v[j, o, 0] = state[:, j * N : (j + 1) * N]
            t_v[j, o, 1] = grad[:, j * N : (j + 1) * N]
        return carry

    for g in range(groups):
        lax.fori_loop(g * per, (g + 1) * per, add_pair, 0)
        piece = pl.ds(g * per, per)
        remote(t_v.at[1 - core, piece], pt_v.at[piece], send_sem.at[5], chunk_sem.at[0, g], partner).start()

    lane_r = lax.broadcasted_iota(jnp.int32, (1, N), 1)

    def decay_of(ref, h):
        return jnp.exp(jnp.sum(jnp.where(lane_r == h, ref[0:1, :], 0.0), axis=1, keepdims=True))

    first = core == 0

    def combine(o, carry):
        h = 2 * o + core
        mine = decay_of(dlo_v, h)
        theirs = decay_of(dlp_v, h)
        one = jnp.ones_like(mine)
        own_f = t_v[core, o, 0].astype(F32)
        own_b = t_v[core, o, 1].astype(F32)
        oth_f = pt_v[o, 0].astype(F32)
        oth_b = pt_v[o, 1].astype(F32)
        state = jnp.where(first, theirs, one) * own_f + jnp.where(first, one, mine) * oth_f
        grad = jnp.where(first, one, theirs) * own_b + jnp.where(first, mine, one) * oth_b
        cb_v[o, 0] = state.astype(BF16)
        cb_v[o, 1] = grad.astype(BF16)
        return carry

    for g in range(groups):
        piece = pl.ds(g * per, per)
        wait_bytes(pt_v.at[piece], chunk_sem.at[0, g])
        lax.fori_loop(g * per, (g + 1) * per, combine, 0)
    for k in range(1, chips):
        other, dev = yz(k)
        remote(cb_v.at[other], rb_v.at[chip], send_sem.at[6], recv_sem.at[6], dev).start()
    rb_v[chip] = cb_v[chip]

    def inner_pair(hp, carry):
        for j in range(2):
            h = hp * 2 + j
            lanes = pl.ds(pl.multiple_of(h * N, N), N)
            col = column(h)
            gain = skip_ref[h]
            for b in range(2):
                rt = col[b * BLOCK : (b + 1) * BLOCK]
                rs = r_v[b, pl.ds(h, 1), :]
                top, bottom = decays(rt, rs)
                top = (top * aff_v[b, 0:half, :]).astype(BF16)
                bottom = (bottom * aff_v[b, half:, half:]).astype(BF16)
                db = dy_v[pl.ds(b * BLOCK, BLOCK), lanes]
                low = db[half:]
                gi_v[pl.ds(b * BLOCK, half), lanes] = (dot_nn(top, db) + gain * db[0:half].astype(F32)).astype(BF16)
                gi_v[pl.ds(b * BLOCK + half, half), lanes] = (dot_nn(bottom, low) + gain * low.astype(F32)).astype(BF16)
        return carry

    lax.fori_loop(0, heads // 2, inner_pair, 0)

    wait_bytes(dc_v.at[pl.ds(0, chips - 1)], recv_sem.at[4])
    wait_bytes(rb_v.at[pl.ds(0, chips - 1)], recv_sem.at[6])
    lane_c = lax.broadcasted_iota(jnp.int32, (chips, N), 1)
    chip_decay = jnp.exp(jnp.sum(jnp.where(lane_c == seq, dc_v[:, 0, :], 0.0), axis=1, keepdims=True))
    run = jnp.zeros((N, N), F32)
    for o in range(chips):
        ob_v[o, 0] = run.astype(BF16)
        run = chip_decay[o : o + 1] * run + rb_v[o, 0].astype(F32)
    run = jnp.zeros((N, N), F32)
    for o in reversed(range(chips)):
        ob_v[o, 1] = run.astype(BF16)
        run = chip_decay[o : o + 1] * run + rb_v[o, 1].astype(F32)
    for k in range(1, chips):
        other, dev = yz(k)
        remote(ob_v.at[other], ib_v.at[chip], send_sem.at[7], recv_sem.at[7], dev).start()
    ib_v[chip] = ob_v[chip]

    for b in range(2):
        at = slice(b * BLOCK, (b + 1) * BLOCK)
        mix = mix_v[b].astype(BF16)
        gbt_v[0:N, at] = dot_nt(bct_v[N:, at], mix)
        gbt_v[N:, at] = dot_nn(bct_v[0:N, at], mix)

    wait_bytes(ib_v.at[pl.ds(0, chips - 1)], recv_sem.at[7])

    def entry(o, carry):
        h = 2 * o + core
        mine = decay_of(dlo_v, h)
        theirs = decay_of(dlp_v, h)
        one = jnp.ones_like(mine)
        nil = jnp.zeros_like(mine)
        state = ib_v[o, 0].astype(F32)
        grad = ib_v[o, 1].astype(F32)
        own_f = t_v[core, o, 0].astype(F32)
        own_b = t_v[core, o, 1].astype(F32)
        oth_f = pt_v[o, 0].astype(F32)
        oth_b = pt_v[o, 1].astype(F32)
        fin_v[core, o, 0] = (jnp.where(first, one, theirs) * state + jnp.where(first, nil, one) * oth_f).astype(BF16)
        fin_v[core, o, 1] = (jnp.where(first, theirs, one) * grad + jnp.where(first, one, nil) * oth_b).astype(BF16)
        xb_v[o, 0] = (jnp.where(first, mine, one) * state + jnp.where(first, one, nil) * own_f).astype(BF16)
        xb_v[o, 1] = (jnp.where(first, one, mine) * grad + jnp.where(first, nil, one) * own_b).astype(BF16)
        return carry

    for g in range(groups):
        lax.fori_loop(g * per, (g + 1) * per, entry, 0)
        piece = pl.ds(g * per, per)
        remote(xb_v.at[piece], fin_v.at[core, piece], send_sem.at[8], chunk_sem.at[1, g], partner).start()

    def finish_pair(o, carry):
        lanes = pl.ds(pl.multiple_of(o * 2 * N, 2 * N), 2 * N)
        e0 = erow_v[0, 0:1, lanes]
        e1 = erow_v[1, 0:1, lanes]
        s0 = jnp.concatenate([fin_v[0, o, 0], fin_v[1, o, 0]], axis=1)
        g1 = jnp.concatenate([fin_v[0, o, 1], fin_v[1, o, 1]], axis=1)
        s1 = (f0_v[:, lanes] + e0 * s0.astype(F32)).astype(BF16)
        g0 = (k1_v[:, lanes] + e1 * g1.astype(F32)).astype(BF16)
        cols = [column(2 * o), column(2 * o + 1)]
        for b, (st, gr) in enumerate(((s0, g0), (s1, g1))):
            at = slice(b * BLOCK, (b + 1) * BLOCK)
            gbt_v[0:N, at] += dot_nt(gr, xs_v[at, lanes])
            gbt_v[N:, at] += dot_nt(st, ds_v[at, lanes])
            outer = dot_nn(bc_v[at, 0:N], gr)
            for j in range(2):
                sub = pl.ds(pl.multiple_of((o * 2 + j) * N, N), N)
                rt = cols[j][at]
                shrink = jnp.exp(rt[BLOCK - 1 : BLOCK] - rt)
                gi_v[at, sub] = (gi_v[at, sub].astype(F32) + shrink * outer[:, j * N : (j + 1) * N]).astype(BF16)
        return carry

    def out_copy(g):
        lanes = pl.ds(g * lanes_g, lanes_g)
        return pltpu.make_async_copy(gi_v.at[:, lanes], gi_hbm.at[:, lanes], out_sem.at[g])

    for g in range(groups):
        piece = pl.ds(g * per, per)
        wait_bytes(xb_v.at[piece], chunk_sem.at[1, g])
        lax.fori_loop(g * per, (g + 1) * per, finish_pair, 0)
        out_copy(g).start()

    gbt_b = gbt_v[...].astype(BF16)

    def weight_pair(o, carry):
        lanes = pl.ds(pl.multiple_of(o * 2 * rblk, 2 * rblk), 2 * rblk)
        part = dot_nn(gbt_b, lay_v[:, lanes]).astype(BF16)
        wg_v[0, o] = part[:, 0:rblk]
        wg_v[1, o] = part[:, rblk:]
        return carry

    for g in range(groups):
        lax.fori_loop(g * per, (g + 1) * per, weight_pair, 0)
        piece = pl.ds(g * per, per)
        remote(wg_v.at[1 - core, piece], rd_v.at[piece], send_sem.at[9], chunk_sem.at[2, g], partner).start()

    def chip_sum(o, carry):
        rss_v[o] = (wg_v[core, o].astype(F32) + rd_v[o].astype(F32)).astype(BF16)
        return carry

    for g in range(groups):
        piece = pl.ds(g * per, per)
        wait_bytes(rd_v.at[piece], chunk_sem.at[2, g])
        lax.fori_loop(g * per, (g + 1) * per, chip_sum, 0)
    for k in range(1, chips):
        other, dev = yz(k)
        remote(rss_v.at[other], rsr_v.at[chip], send_sem.at[10], recv_sem.at[10], dev).start()
    rsr_v[chip] = rss_v[chip]
    wait_bytes(rsr_v.at[pl.ds(0, chips - 1)], recv_sem.at[10])
    acc = rsr_v[0].astype(F32)
    for o in range(1, chips):
        acc = acc + rsr_v[o].astype(F32)
    turned = jnp.transpose(acc)
    for k in range(opts):
        xo_v[k] = turned[k * rows : (k + 1) * rows]
    for k in range(1, opts):
        other, dev = xp(k)
        remote(xo_v.at[other], xr_v.at[opt], send_sem.at[11], recv_sem.at[11], dev).start()
    xr_v[opt] = xo_v[opt]
    wait_bytes(xr_v.at[pl.ds(0, opts - 1)], recv_sem.at[11])
    grad = xr_v[0]
    for k in range(1, opts):
        grad = grad + xr_v[k]

    near = 2 * opts

    def over_all(s1, r1, s2, r2, base, combine_fn):
        me = core * opts + opt
        r1[me] = s1[...]
        for k in range(1, near):
            other = (me + k) % near
            dev = (chip * 2 + other // opts, other % opts)
            remote(s1, r1.at[me], send_sem.at[base], recv_sem.at[base], dev).start()
        wait_bytes(r1.at[pl.ds(0, near - 1)], recv_sem.at[base])
        value = r1[0]
        for k in range(1, near):
            value = combine_fn(value, r1[k])
        s2[...] = value
        r2[chip] = value
        for k in range(1, chips):
            remote(s2, r2.at[chip], send_sem.at[base + 1], recv_sem.at[base + 1], yz(k)[1]).start()
        wait_bytes(r2.at[pl.ds(0, chips - 1)], recv_sem.at[base + 1])
        value = r2[0]
        for k in range(1, chips):
            value = combine_fn(value, r2[k])
        return value

    old_row = rowstat_ref[...]
    a1s_v[0:1, :] = jnp.sum(grad * grad, axis=0, keepdims=True)
    a1s_v[1:8, :] = jnp.broadcast_to(jnp.sum(old_row, axis=1, keepdims=True), (7, 2 * N))
    sums = over_all(a1s_v, a1r_v, a2s_v, a2r_v, 12, jnp.add)
    col_raw = sums[0:1, :]
    old_total = sums[1:2, 0:1]
    raw_total = jnp.sum(col_raw, axis=1, keepdims=True)
    factor = jnp.minimum(1.0, clip_norm / jnp.sqrt(raw_total + norm_floor))
    scaled = grad * factor
    moment = beta_one * code_ref[...].astype(F32) * mscale_ref[...] + (1.0 - beta_one) * scaled
    m1s_v[...] = jnp.broadcast_to(jnp.max(jnp.abs(moment), axis=0, keepdims=True), m1s_v.shape)
    peak = over_all(m1s_v, m1r_v, m2s_v, m2r_v, 14, jnp.maximum)[0:1, :]

    squares = scaled * scaled
    col_next = beta_two * colstat_ref[...] + (1.0 - beta_two) * (factor * factor * col_raw / dim + tiny_square)
    eye = lax.broadcasted_iota(jnp.int32, (rows, rows), 0) == lax.broadcasted_iota(jnp.int32, (rows, rows), 1)
    old_col = jnp.sum(jnp.where(eye, jnp.broadcast_to(old_row, (rows, rows)), 0.0), axis=1, keepdims=True)
    row_next = beta_two * old_col + (1.0 - beta_two) * (
        jnp.sum(squares, axis=1, keepdims=True) / (2 * N) + tiny_square
    )
    row_mean = (
        beta_two * old_total + (1.0 - beta_two) * (factor * factor * raw_total / (2 * N) + dim * tiny_square)
    ) / dim
    second = row_next * col_next / row_mean
    upd_ref[...] = moment / (jnp.sqrt(second) + adam_floor) + weight_decay * w_ref[...]
    scale_next = peak + peak_floor
    scaleo_ref[...] = scale_next
    codeo_ref[...] = (moment / scale_next).astype(BF16)
    colo_ref[...] = col_next
    rowo_ref[...] = jnp.sum(jnp.where(eye, jnp.broadcast_to(row_next, (rows, rows)), 0.0), axis=0, keepdims=True)

    for g in range(groups):
        out_copy(g).wait()
    wait_bytes(w_rows(0, rows * (opts - 1)), send_sem.at[0])
    wait_bytes(dlo_v, send_sem.at[1])
    wait_bytes(w_rows(0, rblk * (chips - 1)), send_sem.at[2])
    wait_bytes(w_rows(0, rblk * chips), send_sem.at[3])
    wait_bytes(dc_v.at[pl.ds(0, chips - 1)], send_sem.at[4])
    wait_bytes(pt_v, send_sem.at[5])
    wait_bytes(cb_v.at[pl.ds(0, chips - 1)], send_sem.at[6])
    wait_bytes(ob_v.at[pl.ds(0, chips - 1)], send_sem.at[7])
    wait_bytes(xb_v, send_sem.at[8])
    wait_bytes(rd_v, send_sem.at[9])
    wait_bytes(rss_v.at[pl.ds(0, chips - 1)], send_sem.at[10])
    wait_bytes(xo_v.at[pl.ds(0, opts - 1)], send_sem.at[11])
    for base, r1, r2 in ((12, a1r_v, a2r_v), (14, m1r_v, m2r_v)):
        wait_bytes(r1.at[pl.ds(0, near - 1)], send_sem.at[base])
        wait_bytes(r2.at[pl.ds(0, chips - 1)], send_sem.at[base + 1])


def per_device(
    seqs, opts, layer_in, ssm_input, grad_out, log_decay, skip_gain, w_bc, m_code, m_scale, row_stat, col_stat
):
    heads = skip_gain.shape[0]
    tokens, width = ssm_input.shape[1:]
    dim = layer_in.shape[2]
    rows = w_bc.shape[0]
    chips = seqs // 2
    rblk = rows * opts
    vm = pl.BlockSpec(memory_space=pltpu.VMEM)
    hbm = pl.BlockSpec(memory_space=pl.ANY)
    state = (chips, 2, N, N)
    scratch = [
        pltpu.VMEM((tokens, width), BF16),
        pltpu.VMEM((tokens, width), BF16),
        pltpu.VMEM((tokens, dim), BF16),
        pltpu.VMEM((tokens, width), BF16),
        pltpu.VMEM((tokens, width), BF16),
        pltpu.VMEM((tokens, width), BF16),
        pltpu.VMEM((dim, 2 * N), BF16),
        pltpu.VMEM((N, tokens), F32),
        pltpu.VMEM((2, N, BLOCK), F32),
        pltpu.VMEM((tokens, N), F32),
        pltpu.VMEM((2, 8, width), F32),
        pltpu.VMEM((2, BLOCK, BLOCK), F32),
        pltpu.VMEM((2, BLOCK, BLOCK), F32),
        pltpu.VMEM((tokens, 2 * N), BF16),
        pltpu.VMEM((2 * N, tokens), BF16),
        pltpu.VMEM((N, width), F32),
        pltpu.VMEM((N, width), F32),
        pltpu.VMEM((2,) + state, BF16),
        pltpu.VMEM(state, BF16),
        pltpu.VMEM(state, BF16),
        pltpu.VMEM(state, BF16),
        pltpu.VMEM(state, BF16),
        pltpu.VMEM(state, BF16),
        pltpu.VMEM(state, BF16),
        pltpu.VMEM((2,) + state, BF16),
        pltpu.VMEM((2 * N, tokens), F32),
        pltpu.VMEM((2, chips, 2 * N, rblk), BF16),
        pltpu.VMEM((chips, 2 * N, rblk), BF16),
        pltpu.VMEM((chips, 2 * N, rblk), BF16),
        pltpu.VMEM((chips, 2 * N, rblk), BF16),
        pltpu.VMEM((opts, rows, 2 * N), F32),
        pltpu.VMEM((opts, rows, 2 * N), F32),
        pltpu.VMEM((8, N), F32),
        pltpu.VMEM((8, N), F32),
        pltpu.VMEM((chips, 8, N), F32),
    ]
    for _ in range(2):
        scratch += [
            pltpu.VMEM((8, 2 * N), F32),
            pltpu.VMEM((2 * opts, 8, 2 * N), F32),
            pltpu.VMEM((8, 2 * N), F32),
            pltpu.VMEM((chips, 8, 2 * N), F32),
        ]
    scratch += [
        pltpu.SemaphoreType.DMA((9,)),
        pltpu.SemaphoreType.DMA((4,)),
        pltpu.SemaphoreType.DMA((16,)),
        pltpu.SemaphoreType.DMA((16,)),
        pltpu.SemaphoreType.DMA((chips,)),
        pltpu.SemaphoreType.DMA((3, 4)),
    ]
    out = pl.pallas_call(
        functools.partial(kernel, seqs, opts),
        out_shape=(
            jax.ShapeDtypeStruct((tokens, width), BF16),
            jax.ShapeDtypeStruct((rows, 2 * N), F32),
            jax.ShapeDtypeStruct((rows, 2 * N), BF16),
            jax.ShapeDtypeStruct((1, 2 * N), F32),
            jax.ShapeDtypeStruct((1, rows), F32),
            jax.ShapeDtypeStruct((1, 2 * N), F32),
        ),
        in_specs=[hbm, hbm, hbm, vm, pl.BlockSpec(memory_space=pltpu.SMEM), vm, vm, vm, vm, vm],
        out_specs=(hbm, vm, vm, vm, vm, vm),
        scratch_shapes=scratch,
        compiler_params=pltpu.CompilerParams(
            collective_id=0, has_side_effects=True, vmem_limit_bytes=66_000_000
        ),
    )(
        ssm_input[0],
        grad_out[0],
        layer_in[0],
        log_decay[0],
        skip_gain,
        w_bc,
        m_code,
        m_scale.reshape(1, 2 * N),
        row_stat.reshape(1, rows),
        col_stat.reshape(1, 2 * N),
    )
    grad_input, update, code_next, scale_next, row_next, col_next = out
    return (
        grad_input[None],
        update,
        code_next,
        scale_next.reshape(2 * N),
        row_next.reshape(rows),
        col_next.reshape(2 * N),
    )


def solution(mesh):
    both = ("seq", "opt")
    return jax.shard_map(
        functools.partial(per_device, mesh.shape["seq"], mesh.shape["opt"]),
        mesh=mesh,
        in_specs=(
            P("opt", "seq", None),
            P("opt", "seq", None),
            P("opt", "seq", None),
            P("opt", None, "seq"),
            P(),
            P(both, None),
            P(both, None),
            P(),
            P(both),
            P(),
        ),
        out_specs=(P("opt", "seq", None), P(both, None), P(both, None), P(), P(both), P()),
        check_vma=False,
    )
```

```python
import functools
import math

import jax
import jax.numpy as jnp
from jax import lax
from jax.experimental import pallas as pl
from jax.experimental.pallas import tpu as pltpu
from jax.sharding import PartitionSpec as P

MESH = pl.DeviceIdType.MESH
BLOCK = 256
N = 128
F32 = jnp.float32
BF16 = jnp.bfloat16
HIGH = lax.Precision.HIGHEST

beta_one = 0.9
beta_two = 0.95
weight_decay = 0.1
clip_norm = 1.0
tiny_square = 1e-30
adam_floor = 1e-08
peak_floor = 1e-06
norm_floor = 1e-06


def dot_nn(a, b, precision=None):
    return lax.dot_general(a, b, (((1,), (0,)), ((), ())), preferred_element_type=F32, precision=precision)


def dot_nt(a, b, precision=None):
    return lax.dot_general(a, b, (((1,), (1,)), ((), ())), preferred_element_type=F32, precision=precision)


def kernel(
    seqs,
    opts,
    x_hbm,
    dy_hbm,
    lay_hbm,
    logs_ref,
    skip_ref,
    w_ref,
    code_ref,
    mscale_ref,
    rowstat_ref,
    colstat_ref,
    gi_hbm,
    upd_ref,
    codeo_ref,
    scaleo_ref,
    rowo_ref,
    colo_ref,
    x_v,
    dy_v,
    lay_v,
    xs_v,
    ds_v,
    gi_v,
    w_v,
    logp_v,
    r_v,
    rt_v,
    erow_v,
    mix_v,
    aff_v,
    bc_v,
    bct_v,
    f0_v,
    k1_v,
    t_v,
    pt_v,
    cb_v,
    rb_v,
    ob_v,
    ib_v,
    xb_v,
    fin_v,
    gbt_v,
    wg_v,
    rd_v,
    rss_v,
    rsr_v,
    xg_v,
    gt_v,
    mc_v,
    rx_v,
    dlo_v,
    dlp_v,
    dc_v,
    s_v,
    m_v,
    in_sem,
    out_sem,
    send_sem,
    recv_sem,
    blk_sem,
    half_sem,
    entry_sem,
    d2d_sem,
    fin_sem,
    rs_sem,
):
    heads = skip_ref.shape[0]
    chips = seqs // 2
    rows = w_ref.shape[0]
    rblk = rows * opts
    width = x_hbm.shape[1]
    dim = lay_hbm.shape[1]
    groups = 4
    lanes_g = width // groups
    fines = min(8, chips)
    fine = chips // fines

    seq = lax.axis_index("seq")
    opt = lax.axis_index("opt")
    chip = seq // 2
    core = seq % 2
    mate = chip * 2 + (1 - core)
    partner = (mate, opt)

    side = math.isqrt(chips)

    def step_of(i):
        return (i * (i + 1) // 2) % side

    def owner_after(e):
        zs = (chip // side + step_of(e // side)) % side
        ys = (chip % side + step_of(e % side)) % side
        return zs * side + ys

    def owner_before(e):
        zs = (chip // side + side - step_of(e // side)) % side
        ys = (chip % side + side - step_of(e % side)) % side
        return zs * side + ys

    def flip(i):
        return 2 * (i % 2) + i // 2 if side == 4 else i

    def opposite(e):
        return flip(e // side) * side + flip(e % side)

    far_first = tuple(range(chips - 1, 0, -1))

    def yz(e):
        other = owner_after(e)
        return other, (other * 2 + core, opt)

    def xp(k):
        other = (opt + k) % opts
        return other, (seq, other)

    def remote(src, dst, s_sem, r_sem, dev):
        return pltpu.make_async_remote_copy(
            src_ref=src, dst_ref=dst, send_sem=s_sem, recv_sem=r_sem, device_id=dev, device_id_type=MESH
        )

    def wait_bytes(ref, sem):
        pltpu.make_async_copy(ref, ref, sem).wait()

    def in_copies(g):
        lanes = pl.ds(g * lanes_g, lanes_g)
        return (
            pltpu.make_async_copy(x_hbm.at[:, lanes], x_v.at[:, lanes], in_sem.at[2 * g]),
            pltpu.make_async_copy(dy_hbm.at[:, lanes], dy_v.at[:, lanes], in_sem.at[2 * g + 1]),
        )

    lay_copy = pltpu.make_async_copy(lay_hbm, lay_v, in_sem.at[2 * groups])

    barrier = pltpu.get_barrier_semaphore()
    for k in range(1, seqs):
        pl.semaphore_signal(barrier, inc=1, device_id=((seq + k) % seqs, opt), device_id_type=MESH)
    for k in range(1, opts):
        pl.semaphore_signal(barrier, inc=1, device_id=xp(k)[1], device_id_type=MESH)

    for g in range(groups):
        for copy in in_copies(g):
            copy.start()
    lay_copy.start()

    w_v[chip, core, opt] = w_ref[...].astype(BF16)
    mc_v[opt] = code_ref[...]
    old_row = rowstat_ref[...]
    rx_v[opt] = jnp.broadcast_to(jnp.sum(old_row, axis=1, keepdims=True), (8, N))

    left = pl.ds(0, N)
    right = pl.ds(N, N)

    def same(ref, s_sem, r_sem, dev):
        return remote(ref, ref, s_sem, r_sem, dev)

    pl.semaphore_wait(barrier, seqs - 1 + opts - 1)
    for k in range(1, opts):
        same(w_v.at[chip, core, opt, :, left], send_sem.at[0], recv_sem.at[0], xp(k)[1]).start()
    for k in far_first:
        same(w_v.at[chip, core, opt, :, right], send_sem.at[12], recv_sem.at[12], yz(k)[1]).start()
    for k in range(1, opts):
        same(rx_v.at[opt], send_sem.at[13], recv_sem.at[13], xp(k)[1]).start()
        same(mc_v.at[opt], send_sem.at[14], recv_sem.at[14], xp(k)[1]).start()

    logp_v[...] = jnp.zeros_like(logp_v)
    logp_v[0:heads, :] = logs_ref[...]
    row_i = lax.broadcasted_iota(jnp.int32, (BLOCK, BLOCK), 0)
    col_i = lax.broadcasted_iota(jnp.int32, (BLOCK, BLOCK), 1)
    upper = jnp.where(row_i <= col_i, 1.0, 0.0).astype(F32)
    lower = jnp.where(row_i >= col_i, 1.0, 0.0).astype(F32)
    for b in range(2):
        part = logp_v[:, b * BLOCK : (b + 1) * BLOCK]
        r_v[b] = dot_nn(part, upper, HIGH)
        rt_v[b * BLOCK : (b + 1) * BLOCK, :] = dot_nt(lower, part, HIGH)

    mix_v[...] = jnp.zeros_like(mix_v)
    lane_i = lax.broadcasted_iota(jnp.int32, (2 * BLOCK, N), 1)

    def column(h):
        return jnp.sum(jnp.where(lane_i == h, rt_v[...], 0.0), axis=1, keepdims=True)

    half = BLOCK // 2
    tri_a = lax.broadcasted_iota(jnp.int32, (half, BLOCK), 1) >= lax.broadcasted_iota(jnp.int32, (half, BLOCK), 0)
    tri_b = lax.broadcasted_iota(jnp.int32, (half, half), 1) >= lax.broadcasted_iota(jnp.int32, (half, half), 0)

    def decays(rt, rs):
        top = jnp.exp(jnp.where(tri_a, rs - rt[0:half], -jnp.inf))
        bottom = jnp.exp(jnp.where(tri_b, rs[:, half:] - rt[half:], -jnp.inf))
        return top, bottom

    def mix_pair(hp, carry):
        adds = [[None, None], [None, None]]
        for j in range(2):
            h = hp * 2 + j
            lanes = pl.ds(pl.multiple_of(h * N, N), N)
            col = column(h)
            for b in range(2):
                at = pl.ds(b * BLOCK, BLOCK)
                xb = x_v[at, lanes]
                db = dy_v[at, lanes]
                rt = col[b * BLOCK : (b + 1) * BLOCK]
                rs = r_v[b, pl.ds(h, 1), :]
                prod = dot_nt(xb, db)
                top, bottom = decays(rt, rs)
                top = top * prod[0:half]
                bottom = bottom * prod[half:, half:]
                adds[b][0] = top if j == 0 else adds[b][0] + top
                adds[b][1] = bottom if j == 0 else adds[b][1] + bottom
                closing = rt[BLOCK - 1 : BLOCK]
                erow_v[b, :, lanes] = jnp.broadcast_to(jnp.exp(closing), (8, N))
                xs_v[at, lanes] = (xb.astype(F32) * jnp.exp(closing - rt)).astype(BF16)
                ds_v[at, lanes] = (db.astype(F32) * jnp.exp(rt)).astype(BF16)
        for b in range(2):
            mix_v[b, 0:half, :] += adds[b][0]
            mix_v[b, half:, half:] += adds[b][1]
        return carry

    pairs = heads // 2

    def mix_group(first_pair, last_pair):
        for g in range(groups):
            if first_pair <= g * (pairs // groups) < last_pair:
                for copy in in_copies(g):
                    copy.wait()
        lax.fori_loop(first_pair, last_pair, mix_pair, 0)

    cuts = (0, pairs // 8, pairs // 4, pairs * 3 // 8, pairs)
    mix_group(cuts[0], cuts[1])
    wait_bytes(w_v.at[0, 0, pl.ds(0, opts - 1), :, left], recv_sem.at[0])
    for k in far_first:
        same(w_v.at[chip, core, :, :, left], send_sem.at[2], blk_sem.at[k], yz(k)[1]).start()
    same(w_v.at[chip, core, :, :, left], send_sem.at[3], recv_sem.at[3], partner).start()
    wait_bytes(rx_v.at[pl.ds(0, opts - 1)], recv_sem.at[13])
    old_sum = rx_v[0]
    for k in range(1, opts):
        old_sum = old_sum + rx_v[k]
    dlo_v[...] = old_sum
    dlo_v[0:1, :] = rt_v[BLOCK - 1 : BLOCK, :] + rt_v[2 * BLOCK - 1 : 2 * BLOCK, :]
    remote(dlo_v, dlp_v, send_sem.at[1], recv_sem.at[1], partner).start()
    mix_group(cuts[1], cuts[2])
    wait_bytes(w_v.at[pl.ds(0, chips - 1), 0, 0, :, right], recv_sem.at[12])
    for k in range(1, opts):
        same(w_v.at[:, core, opt, :, right], send_sem.at[15], half_sem.at[k], xp(k)[1]).start()
    same(w_v.at[:, core, opt, :, right], send_sem.at[3], recv_sem.at[3], partner).start()
    mix_group(cuts[2], cuts[3])
    wait_bytes(dlp_v, recv_sem.at[1])
    dc_v[chip] = dlo_v[...] + dlp_v[...]
    for k in far_first:
        same(dc_v.at[chip], send_sem.at[4], recv_sem.at[4], yz(k)[1]).start()
    mix_group(cuts[3], cuts[4])
    for k in range(1, chips):
        block = w_v.at[owner_before(k), core, :, :, left]
        wait_bytes(block, blk_sem.at[k])
        same(block, send_sem.at[3], recv_sem.at[3], partner).start()
    for k in range(1, opts):
        block = w_v.at[:, core, (opt + opts - k) % opts, :, right]
        wait_bytes(block, half_sem.at[k])
        same(block, send_sem.at[3], recv_sem.at[3], partner).start()
    lay_copy.wait()
    wait_bytes(w_v.at[:, 0], recv_sem.at[3])

    proj = dot_nn(lay_v[...], w_v[...].reshape(dim, 2 * N)).astype(BF16)
    bc_v[...] = proj
    bct_v[...] = jnp.transpose(proj.astype(F32)).astype(BF16)
    for b in range(2):
        at = slice(b * BLOCK, (b + 1) * BLOCK)
        aff_v[b] = dot_nt(bc_v[at, 0:N], bc_v[at, N : 2 * N])

    def add_pair(k, carry):
        lanes = pl.ds(pl.multiple_of(owner_after(k) * 2 * N, 2 * N), 2 * N)
        e0 = erow_v[0, 0:1, lanes]
        e1 = erow_v[1, 0:1, lanes]
        f0 = dot_nn(bct_v[0:N, 0:BLOCK], xs_v[0:BLOCK, lanes])
        f1 = dot_nn(bct_v[0:N, BLOCK:], xs_v[BLOCK:, lanes])
        k0 = dot_nn(bct_v[N:, 0:BLOCK], ds_v[0:BLOCK, lanes])
        k1 = dot_nn(bct_v[N:, BLOCK:], ds_v[BLOCK:, lanes])
        f0_v[:, lanes] = f0
        k1_v[:, lanes] = k1
        state = (e1 * f0 + f1).astype(BF16)
        grad = (k0 + e0 * k1).astype(BF16)
        for j in range(2):
            t_v[j, k, 0] = state[:, j * N : (j + 1) * N]
            t_v[j, k, 1] = grad[:, j * N : (j + 1) * N]
        return carry

    lane_r = lax.broadcasted_iota(jnp.int32, (1, N), 1)

    def decay_of(ref, h):
        return jnp.exp(jnp.sum(jnp.where(lane_r == h, ref[0:1, :], 0.0), axis=1, keepdims=True))

    first = core == 0

    def combine(k, carry):
        h = 2 * owner_after(k) + core
        mine = decay_of(dlo_v, h)
        theirs = decay_of(dlp_v, h)
        one = jnp.ones_like(mine)
        own_f = t_v[core, k, 0].astype(F32)
        own_b = t_v[core, k, 1].astype(F32)
        oth_f = pt_v[k, 0].astype(F32)
        oth_b = pt_v[k, 1].astype(F32)
        state = jnp.where(first, theirs, one) * own_f + jnp.where(first, one, mine) * oth_f
        grad = jnp.where(first, one, theirs) * own_b + jnp.where(first, mine, one) * oth_b
        cb_v[k, 0] = state.astype(BF16)
        cb_v[k, 1] = grad.astype(BF16)
        return carry

    def piece(g):
        return chips - (g + 1) * fine

    def combine_group(g):
        at = pl.ds(piece(g), fine)
        wait_bytes(pt_v.at[at], d2d_sem.at[g])
        lax.fori_loop(piece(g), piece(g) + fine, combine, 0, unroll=True)
        for k in reversed(range(max(1, piece(g)), piece(g) + fine)):
            remote(cb_v.at[k], rb_v.at[chip], send_sem.at[6], recv_sem.at[6], yz(k)[1]).start()

    lag = 2
    for g in range(fines):
        lax.fori_loop(piece(g), piece(g) + fine, add_pair, 0, unroll=True)
        at = pl.ds(piece(g), fine)
        remote(t_v.at[1 - core, at], pt_v.at[at], send_sem.at[5], d2d_sem.at[g], partner).start()
        if g >= lag:
            combine_group(g - lag)
    for g in range(max(0, fines - lag), fines):
        combine_group(g)
    rb_v[chip] = cb_v[0]

    def inner_pair(hp, carry):
        for j in range(2):
            h = hp * 2 + j
            lanes = pl.ds(pl.multiple_of(h * N, N), N)
            col = column(h)
            gain = skip_ref[h]
            for b in range(2):
                rt = col[b * BLOCK : (b + 1) * BLOCK]
                rs = r_v[b, pl.ds(h, 1), :]
                top, bottom = decays(rt, rs)
                top = (top * aff_v[b, 0:half, :]).astype(BF16)
                bottom = (bottom * aff_v[b, half:, half:]).astype(BF16)
                db = dy_v[pl.ds(b * BLOCK, BLOCK), lanes]
                low = db[half:]
                gi_v[pl.ds(b * BLOCK, half), lanes] = (dot_nn(top, db) + gain * db[0:half].astype(F32)).astype(BF16)
                gi_v[pl.ds(b * BLOCK + half, half), lanes] = (dot_nn(bottom, low) + gain * low.astype(F32)).astype(BF16)
        return carry

    lax.fori_loop(0, heads // 2, inner_pair, 0)

    wait_bytes(dc_v.at[pl.ds(0, chips - 1)], recv_sem.at[4])
    wait_bytes(rb_v.at[pl.ds(0, chips - 1)], recv_sem.at[6])
    lane_c = lax.broadcasted_iota(jnp.int32, (chips, N), 1)
    chip_decay = jnp.exp(jnp.sum(jnp.where(lane_c == seq, dc_v[:, 0, :], 0.0), axis=1, keepdims=True))
    run = jnp.zeros((N, N), F32)
    for o in range(chips):
        ob_v[o, 0] = run.astype(BF16)
        run = chip_decay[o : o + 1] * run + rb_v[o, 0].astype(F32)
    run = jnp.zeros((N, N), F32)
    for o in reversed(range(chips)):
        ob_v[o, 1] = run.astype(BF16)
        run = chip_decay[o : o + 1] * run + rb_v[o, 1].astype(F32)
    for k in range(1, chips):
        other, dev = yz(k)
        remote(ob_v.at[other], ib_v.at[k], send_sem.at[7], entry_sem.at[k], dev).start()
    ib_v[0] = ob_v[chip]

    for b in range(2):
        at = slice(b * BLOCK, (b + 1) * BLOCK)
        mix = mix_v[b].astype(BF16)
        gbt_v[0:N, at] = dot_nt(bct_v[N:, at], mix)
        gbt_v[N:, at] = dot_nn(bct_v[0:N, at], mix)

    def entry(k, carry):
        h = 2 * owner_before(k) + core
        back = opposite(k)
        mine = decay_of(dlo_v, h)
        theirs = decay_of(dlp_v, h)
        one = jnp.ones_like(mine)
        nil = jnp.zeros_like(mine)
        state = ib_v[k, 0].astype(F32)
        grad = ib_v[k, 1].astype(F32)
        own_f = t_v[core, back, 0].astype(F32)
        own_b = t_v[core, back, 1].astype(F32)
        oth_f = pt_v[back, 0].astype(F32)
        oth_b = pt_v[back, 1].astype(F32)
        fin_v[core, k, 0] = (jnp.where(first, one, theirs) * state + jnp.where(first, nil, one) * oth_f).astype(BF16)
        fin_v[core, k, 1] = (jnp.where(first, theirs, one) * grad + jnp.where(first, one, nil) * oth_b).astype(BF16)
        xb_v[k, 0] = (jnp.where(first, mine, one) * state + jnp.where(first, one, nil) * own_f).astype(BF16)
        xb_v[k, 1] = (jnp.where(first, one, mine) * grad + jnp.where(first, nil, one) * own_b).astype(BF16)
        return carry

    def finish_pair(k, carry):
        o = owner_before(k)
        lanes = pl.ds(pl.multiple_of(o * 2 * N, 2 * N), 2 * N)
        e0 = erow_v[0, 0:1, lanes]
        e1 = erow_v[1, 0:1, lanes]
        s0 = jnp.concatenate([fin_v[0, k, 0], fin_v[1, k, 0]], axis=1)
        g1 = jnp.concatenate([fin_v[0, k, 1], fin_v[1, k, 1]], axis=1)
        s1 = (f0_v[:, lanes] + e0 * s0.astype(F32)).astype(BF16)
        g0 = (k1_v[:, lanes] + e1 * g1.astype(F32)).astype(BF16)
        cols = [column(2 * o), column(2 * o + 1)]
        for b, (st, gr) in enumerate(((s0, g0), (s1, g1))):
            at = slice(b * BLOCK, (b + 1) * BLOCK)
            gbt_v[0:N, at] += dot_nt(gr, xs_v[at, lanes])
            gbt_v[N:, at] += dot_nt(st, ds_v[at, lanes])
            outer = dot_nn(bc_v[at, 0:N], gr)
            for j in range(2):
                sub = pl.ds(pl.multiple_of((o * 2 + j) * N, N), N)
                rt = cols[j][at]
                shrink = jnp.exp(rt[BLOCK - 1 : BLOCK] - rt)
                gi_v[at, sub] = (gi_v[at, sub].astype(F32) + shrink * outer[:, j * N : (j + 1) * N]).astype(BF16)
        return carry

    def out_copy(k):
        lanes = pl.ds(pl.multiple_of(owner_before(k) * 2 * N, 2 * N), 2 * N)
        return pltpu.make_async_copy(gi_v.at[:, lanes], gi_hbm.at[:, lanes], out_sem.at[k])

    def finish_group(g):
        wait_bytes(xb_v.at[pl.ds(g * fine, fine)], fin_sem.at[g])
        lax.fori_loop(g * fine, (g + 1) * fine, finish_pair, 0, unroll=True)
        for k in range(g * fine, (g + 1) * fine):
            out_copy(k).start()

    for g in range(fines):
        at = pl.ds(g * fine, fine)
        for k in range(max(1, g * fine), (g + 1) * fine):
            wait_bytes(ib_v.at[k], entry_sem.at[k])
        lax.fori_loop(g * fine, (g + 1) * fine, entry, 0, unroll=True)
        remote(xb_v.at[at], fin_v.at[core, at], send_sem.at[8], fin_sem.at[g], partner).start()
        if g >= 1:
            finish_group(g - 1)
    finish_group(fines - 1)

    gbt_b = gbt_v[...].astype(BF16)

    def weight_pair(k, carry):
        lanes = pl.ds(pl.multiple_of(owner_after(k) * 2 * rblk, 2 * rblk), 2 * rblk)
        part = dot_nn(gbt_b, lay_v[:, lanes]).astype(BF16)
        wg_v[0, k] = part[:, 0:rblk]
        wg_v[1, k] = part[:, rblk:]
        return carry

    def chip_sum(k, carry):
        rss_v[k] = (wg_v[core, k].astype(F32) + rd_v[k].astype(F32)).astype(BF16)
        return carry

    def sum_group(g):
        at = pl.ds(piece(g), fine)
        wait_bytes(rd_v.at[at], rs_sem.at[g])
        lax.fori_loop(piece(g), piece(g) + fine, chip_sum, 0, unroll=True)
        for k in reversed(range(max(1, piece(g)), piece(g) + fine)):
            remote(rss_v.at[k], rsr_v.at[k], send_sem.at[10], recv_sem.at[10], yz(k)[1]).start()

    for g in range(fines):
        lax.fori_loop(piece(g), piece(g) + fine, weight_pair, 0, unroll=True)
        at = pl.ds(piece(g), fine)
        remote(wg_v.at[1 - core, at], rd_v.at[at], send_sem.at[9], rs_sem.at[g], partner).start()
        if g >= lag:
            sum_group(g - lag)
    for g in range(max(0, fines - lag), fines):
        sum_group(g)
    rsr_v[0] = rss_v[0]
    wait_bytes(rsr_v.at[pl.ds(0, chips - 1)], recv_sem.at[10])
    acc = rsr_v[0].astype(F32)
    for k in range(1, chips):
        acc = acc + rsr_v[k].astype(F32)
    xg_v[opt] = jnp.transpose(acc).astype(BF16)
    for k in range(1, opts):
        same(xg_v.at[opt], send_sem.at[11], recv_sem.at[11], xp(k)[1]).start()
    wait_bytes(mc_v.at[pl.ds(0, opts - 1)], recv_sem.at[14])
    wait_bytes(xg_v.at[pl.ds(0, opts - 1)], recv_sem.at[11])
    grad = xg_v[0].astype(F32)
    for k in range(1, opts):
        grad = grad + xg_v[k].astype(F32)
    gt_v[...] = grad

    def over_all(buf, row, base, combine_fn):
        buf[seq, 0:1] = row
        for k in range(1, seqs):
            same(buf.at[seq, 0:1], send_sem.at[base], recv_sem.at[base], ((seq + k) % seqs, opt)).start()
        wait_bytes(buf.at[pl.ds(0, seqs - 1), 0:1], recv_sem.at[base])
        value = buf[0, 0:1]
        for k in range(1, seqs):
            value = combine_fn(value, buf[k, 0:1])
        return value

    col_raw = over_all(s_v, jnp.sum(grad * grad, axis=0, keepdims=True), 16, jnp.add)
    raw_total = jnp.sum(col_raw, axis=1, keepdims=True)
    factor = jnp.minimum(1.0, clip_norm / jnp.sqrt(raw_total + norm_floor))

    def moment_of(code, part):
        return beta_one * code.astype(F32) * mscale_ref[...] + (1.0 - beta_one) * (part * factor)

    top = jnp.zeros((1, 2 * N), F32)
    for k in range(opts):
        part = moment_of(mc_v[k], gt_v[k * rows : (k + 1) * rows])
        top = jnp.maximum(top, jnp.max(jnp.abs(part), axis=0, keepdims=True))
    peak = over_all(m_v, top, 17, jnp.maximum)

    own = gt_v[pl.ds(pl.multiple_of(opt * rows, rows), rows), :]
    scaled = own * factor
    moment = moment_of(code_ref[...], own)
    squares = scaled * scaled
    old_total = jnp.sum(dc_v[:, 1, 0:1], axis=0, keepdims=True)
    col_next = beta_two * colstat_ref[...] + (1.0 - beta_two) * (factor * factor * col_raw / dim + tiny_square)
    eye = lax.broadcasted_iota(jnp.int32, (rows, rows), 0) == lax.broadcasted_iota(jnp.int32, (rows, rows), 1)
    old_col = jnp.sum(jnp.where(eye, jnp.broadcast_to(old_row, (rows, rows)), 0.0), axis=1, keepdims=True)
    row_next = beta_two * old_col + (1.0 - beta_two) * (
        jnp.sum(squares, axis=1, keepdims=True) / (2 * N) + tiny_square
    )
    row_mean = (
        beta_two * old_total + (1.0 - beta_two) * (factor * factor * raw_total / (2 * N) + dim * tiny_square)
    ) / dim
    second = row_next * col_next / row_mean
    upd_ref[...] = moment / (jnp.sqrt(second) + adam_floor) + weight_decay * w_ref[...]
    scale_next = peak + peak_floor
    scaleo_ref[...] = scale_next
    codeo_ref[...] = (moment / scale_next).astype(BF16)
    colo_ref[...] = col_next
    rowo_ref[...] = jnp.sum(jnp.where(eye, jnp.broadcast_to(row_next, (rows, rows)), 0.0), axis=0, keepdims=True)

    for k in range(chips):
        out_copy(k).wait()
    wait_bytes(w_v.at[0, 0, pl.ds(0, opts - 1), :, left], send_sem.at[0])
    wait_bytes(dlo_v, send_sem.at[1])
    wait_bytes(w_v.at[pl.ds(0, chips - 1), 0, :, :, left], send_sem.at[2])
    wait_bytes(w_v.at[:, 0], send_sem.at[3])
    wait_bytes(dc_v.at[pl.ds(0, chips - 1)], send_sem.at[4])
    wait_bytes(pt_v, send_sem.at[5])
    wait_bytes(cb_v.at[pl.ds(0, chips - 1)], send_sem.at[6])
    wait_bytes(ob_v.at[pl.ds(0, chips - 1)], send_sem.at[7])
    wait_bytes(xb_v, send_sem.at[8])
    wait_bytes(rd_v, send_sem.at[9])
    wait_bytes(rss_v.at[pl.ds(0, chips - 1)], send_sem.at[10])
    wait_bytes(xg_v.at[pl.ds(0, opts - 1)], send_sem.at[11])
    wait_bytes(w_v.at[pl.ds(0, chips - 1), 0, 0, :, right], send_sem.at[12])
    wait_bytes(rx_v.at[pl.ds(0, opts - 1)], send_sem.at[13])
    wait_bytes(mc_v.at[pl.ds(0, opts - 1)], send_sem.at[14])
    wait_bytes(w_v.at[:, 0, pl.ds(0, opts - 1), :, right], send_sem.at[15])
    for base, buf in ((16, s_v), (17, m_v)):
        wait_bytes(buf.at[pl.ds(0, seqs - 1), 0:1], send_sem.at[base])


def copy_out(gi_hbm, upd_ref, code_ref, scale_ref, row_ref, col_ref, gi_out, upd_o, code_o, scale_o, row_o, col_o, held, i_sem, o_sem):
    pieces = i_sem.shape[0]
    size = held.shape[0] // pieces

    def move(source, target, k, sem):
        at = pl.ds(k * size, size)
        return pltpu.make_async_copy(source.at[at], target.at[at], sem.at[k])

    for k in range(pieces):
        move(gi_hbm, held, k, i_sem).start()
    upd_o[...] = upd_ref[...]
    code_o[...] = code_ref[...]
    scale_o[...] = scale_ref[...]
    row_o[...] = row_ref[...]
    col_o[...] = col_ref[...]
    for k in range(pieces):
        move(gi_hbm, held, k, i_sem).wait()
        move(held, gi_out, k, o_sem).start()
    for k in range(pieces):
        move(held, gi_out, k, o_sem).wait()


def per_device(
    seqs, opts, layer_in, ssm_input, grad_out, log_decay, skip_gain, w_bc, m_code, m_scale, row_stat, col_stat
):
    heads = skip_gain.shape[0]
    tokens, width = ssm_input.shape[1:]
    dim = layer_in.shape[2]
    rows = w_bc.shape[0]
    chips = seqs // 2
    rblk = rows * opts
    vm = pl.BlockSpec(memory_space=pltpu.VMEM)
    hbm = pl.BlockSpec(memory_space=pl.ANY)
    state = (chips, 2, N, N)
    scratch = [
        pltpu.VMEM((tokens, width), BF16),
        pltpu.VMEM((tokens, width), BF16),
        pltpu.VMEM((tokens, dim), BF16),
        pltpu.VMEM((tokens, width), BF16),
        pltpu.VMEM((tokens, width), BF16),
        pltpu.VMEM((tokens, width), BF16),
        pltpu.VMEM((chips, 2, opts, rows, 2 * N), BF16),
        pltpu.VMEM((N, tokens), F32),
        pltpu.VMEM((2, N, BLOCK), F32),
        pltpu.VMEM((tokens, N), F32),
        pltpu.VMEM((2, 8, width), F32),
        pltpu.VMEM((2, BLOCK, BLOCK), F32),
        pltpu.VMEM((2, BLOCK, BLOCK), F32),
        pltpu.VMEM((tokens, 2 * N), BF16),
        pltpu.VMEM((2 * N, tokens), BF16),
        pltpu.VMEM((N, width), F32),
        pltpu.VMEM((N, width), F32),
        pltpu.VMEM((2,) + state, BF16),
        pltpu.VMEM(state, BF16),
        pltpu.VMEM(state, BF16),
        pltpu.VMEM(state, BF16),
        pltpu.VMEM(state, BF16),
        pltpu.VMEM(state, BF16),
        pltpu.VMEM(state, BF16),
        pltpu.VMEM((2,) + state, BF16),
        pltpu.VMEM((2 * N, tokens), F32),
        pltpu.VMEM((2, chips, 2 * N, rblk), BF16),
        pltpu.VMEM((chips, 2 * N, rblk), BF16),
        pltpu.VMEM((chips, 2 * N, rblk), BF16),
        pltpu.VMEM((chips, 2 * N, rblk), BF16),
        pltpu.VMEM((opts, rblk, 2 * N), BF16),
        pltpu.VMEM((rblk, 2 * N), F32),
        pltpu.VMEM((opts, rows, 2 * N), BF16),
        pltpu.VMEM((opts, 8, N), F32),
        pltpu.VMEM((8, N), F32),
        pltpu.VMEM((8, N), F32),
        pltpu.VMEM((chips, 8, N), F32),
        pltpu.VMEM((seqs, 8, 2 * N), F32),
        pltpu.VMEM((seqs, 8, 2 * N), F32),
        pltpu.SemaphoreType.DMA((9,)),
        pltpu.SemaphoreType.DMA((chips,)),
        pltpu.SemaphoreType.DMA((18,)),
        pltpu.SemaphoreType.DMA((18,)),
        pltpu.SemaphoreType.DMA((chips,)),
        pltpu.SemaphoreType.DMA((opts,)),
        pltpu.SemaphoreType.DMA((chips,)),
        pltpu.SemaphoreType.DMA((min(8, chips),)),
        pltpu.SemaphoreType.DMA((min(8, chips),)),
        pltpu.SemaphoreType.DMA((min(8, chips),)),
    ]
    shapes = (
        jax.ShapeDtypeStruct((tokens, width), BF16),
        jax.ShapeDtypeStruct((rows, 2 * N), F32),
        jax.ShapeDtypeStruct((rows, 2 * N), BF16),
        jax.ShapeDtypeStruct((1, 2 * N), F32),
        jax.ShapeDtypeStruct((1, rows), F32),
        jax.ShapeDtypeStruct((1, 2 * N), F32),
    )
    out = pl.pallas_call(
        functools.partial(kernel, seqs, opts),
        out_shape=shapes,
        in_specs=[hbm, hbm, hbm, vm, pl.BlockSpec(memory_space=pltpu.SMEM), vm, vm, vm, vm, vm],
        out_specs=(hbm, vm, vm, vm, vm, vm),
        scratch_shapes=scratch,
        compiler_params=pltpu.CompilerParams(
            collective_id=0, has_side_effects=True, vmem_limit_bytes=66_000_000
        ),
    )(
        ssm_input[0],
        grad_out[0],
        layer_in[0],
        log_decay[0],
        skip_gain,
        w_bc,
        m_code,
        m_scale.reshape(1, 2 * N),
        row_stat.reshape(1, rows),
        col_stat.reshape(1, 2 * N),
    )
    out = pl.pallas_call(
        copy_out,
        out_shape=shapes,
        in_specs=[hbm, vm, vm, vm, vm, vm],
        out_specs=(hbm, vm, vm, vm, vm, vm),
        scratch_shapes=[
            pltpu.VMEM((tokens, width), BF16),
            pltpu.SemaphoreType.DMA((8,)),
            pltpu.SemaphoreType.DMA((8,)),
        ],
    )(*out)
    grad_input, update, code_next, scale_next, row_next, col_next = out
    return (
        grad_input[None],
        update,
        code_next,
        scale_next.reshape(2 * N),
        row_next.reshape(rows),
        col_next.reshape(2 * N),
    )


def solution(mesh):
    both = ("seq", "opt")
    return jax.shard_map(
        functools.partial(per_device, mesh.shape["seq"], mesh.shape["opt"]),
        mesh=mesh,
        in_specs=(
            P("opt", "seq", None),
            P("opt", "seq", None),
            P("opt", "seq", None),
            P("opt", None, "seq"),
            P(),
            P(both, None),
            P(both, None),
            P(),
            P(both),
            P(),
        ),
        out_specs=(P("opt", "seq", None), P(both, None), P(both, None), P(), P(both), P()),
        check_vma=False,
    )
```

```python
import functools
import math

import jax
import jax.numpy as jnp
from jax import lax
from jax.experimental import pallas as pl
from jax.experimental.pallas import tpu as pltpu
from jax.sharding import PartitionSpec as P

MESH = pl.DeviceIdType.MESH
BLOCK = 256
N = 128
F32 = jnp.float32
BF16 = jnp.bfloat16
HIGH = lax.Precision.HIGHEST

beta_one = 0.9
beta_two = 0.95
weight_decay = 0.1
clip_norm = 1.0
tiny_square = 1e-30
adam_floor = 1e-08
peak_floor = 1e-06
norm_floor = 1e-06


def dot_nn(a, b, precision=None):
    return lax.dot_general(a, b, (((1,), (0,)), ((), ())), preferred_element_type=F32, precision=precision)


def dot_nt(a, b, precision=None):
    return lax.dot_general(a, b, (((1,), (1,)), ((), ())), preferred_element_type=F32, precision=precision)


def kernel(
    seqs,
    opts,
    x_hbm,
    dy_hbm,
    lay_hbm,
    logs_hbm,
    skip_hbm,
    w_hbm,
    code_hbm,
    mscale_hbm,
    rowstat_hbm,
    colstat_hbm,
    gi_v,
    upd_ref,
    codeo_ref,
    scaleo_ref,
    rowo_ref,
    colo_ref,
    x_v,
    dy_v,
    lay_v,
    xs_v,
    ds_v,
    wl_v,
    wr_v,
    logp_v,
    skip_ref,
    w_ref,
    mscale_ref,
    rowstat_ref,
    colstat_ref,
    r_v,
    rt_v,
    erow_v,
    mix_v,
    aff_v,
    bc_v,
    bct_v,
    f0_v,
    k1_v,
    t_v,
    pt_v,
    cb_v,
    rb_v,
    ob_v,
    ib_v,
    xb_v,
    fin_v,
    gbt_v,
    wg_v,
    rd_v,
    rss_v,
    rsr_v,
    bx_v,
    by_v,
    bz_v,
    bw_v,
    xg_v,
    gt_v,
    mc_v,
    rx_v,
    dlo_v,
    dlp_v,
    dc_v,
    s_v,
    m_v,
    in_sem,
    small_sem,
    send_sem,
    recv_sem,
    blk_sem,
    half_sem,
    entry_sem,
    d2d_sem,
    fin_sem,
    rs_sem,
):
    heads = skip_ref.shape[1]
    chips = seqs // 2
    rows = w_ref.shape[0]
    rblk = rows * opts
    width = x_hbm.shape[1]
    dim = lay_hbm.shape[1]
    groups = 4
    lanes_g = width // groups
    fines = min(8, chips)
    fine = chips // fines
    parts = 4
    per = chips // parts

    seq = lax.axis_index("seq")
    opt = lax.axis_index("opt")
    chip = seq // 2
    core = seq % 2
    mate = chip * 2 + (1 - core)
    partner = (mate, opt)

    side = math.isqrt(chips)

    def step_of(i):
        return (i * (i + 1) // 2) % side

    def owner_after(e):
        zs = (chip // side + step_of(e // side)) % side
        ys = (chip % side + step_of(e % side)) % side
        return zs * side + ys

    def owner_before(e):
        zs = (chip // side + side - step_of(e // side)) % side
        ys = (chip % side + side - step_of(e % side)) % side
        return zs * side + ys

    def flip(i):
        return 2 * (i % 2) + i // 2 if side == 4 else i

    def opposite(e):
        return flip(e // side) * side + flip(e % side)

    far_first = tuple(range(chips - 1, 0, -1))

    def yz(e):
        other = owner_after(e)
        return other, (other * 2 + core, opt)

    def xp(k):
        other = (opt + k) % opts
        return other, (seq, other)

    def remote(src, dst, s_sem, r_sem, dev):
        return pltpu.make_async_remote_copy(
            src_ref=src, dst_ref=dst, send_sem=s_sem, recv_sem=r_sem, device_id=dev, device_id_type=MESH
        )

    def wait_bytes(ref, sem):
        pltpu.make_async_copy(ref, ref, sem).wait()

    def in_copies(g):
        lanes = pl.ds(g * lanes_g, lanes_g)
        return (
            pltpu.make_async_copy(x_hbm.at[:, lanes], x_v.at[:, lanes], in_sem.at[2 * g]),
            pltpu.make_async_copy(dy_hbm.at[:, lanes], dy_v.at[:, lanes], in_sem.at[2 * g + 1]),
        )

    lay_copy = pltpu.make_async_copy(lay_hbm, lay_v, in_sem.at[2 * groups])

    barrier = pltpu.get_barrier_semaphore()
    for k in range(1, seqs):
        pl.semaphore_signal(barrier, inc=1, device_id=((seq + k) % seqs, opt), device_id_type=MESH)
    for k in range(1, opts):
        pl.semaphore_signal(barrier, inc=1, device_id=xp(k)[1], device_id_type=MESH)

    def small(source, target, k):
        return pltpu.make_async_copy(source, target, small_sem.at[k])

    smalls = [
        small(w_hbm, w_ref, 0),
        small(rowstat_hbm, rowstat_ref, 1),
        small(code_hbm, mc_v.at[opt], 2),
        small(logs_hbm, logp_v.at[pl.ds(0, heads)], 3),
        small(skip_hbm, skip_ref, 4),
        small(mscale_hbm, mscale_ref, 5),
        small(colstat_hbm, colstat_ref, 6),
    ]
    for copy in smalls:
        copy.start()
    for g in range(groups):
        for copy in in_copies(g):
            copy.start()
    lay_copy.start()
    if heads < N:
        logp_v[heads:, :] = jnp.zeros((N - heads, logp_v.shape[1]), F32)

    for copy in smalls:
        copy.wait()
    wl_v[chip, core, opt] = w_ref[:, 0:N].astype(BF16)
    wr_v[chip, core, opt] = w_ref[:, N:].astype(BF16)
    old_row = rowstat_ref[...]
    rx_v[opt] = jnp.broadcast_to(jnp.sum(old_row, axis=1, keepdims=True), (8, N))


    def same(ref, s_sem, r_sem, dev):
        return remote(ref, ref, s_sem, r_sem, dev)

    pl.semaphore_wait(barrier, seqs - 1 + opts - 1)
    for k in range(1, opts):
        same(wl_v.at[chip, core, opt], send_sem.at[0], recv_sem.at[0], xp(k)[1]).start()
    for k in far_first:
        same(wr_v.at[chip, core, opt], send_sem.at[12], recv_sem.at[12], yz(k)[1]).start()
    for k in range(1, opts):
        same(rx_v.at[opt], send_sem.at[13], recv_sem.at[13], xp(k)[1]).start()
        same(mc_v.at[opt], send_sem.at[14], recv_sem.at[14], xp(k)[1]).start()

    row_i = lax.broadcasted_iota(jnp.int32, (BLOCK, BLOCK), 0)
    col_i = lax.broadcasted_iota(jnp.int32, (BLOCK, BLOCK), 1)
    upper = jnp.where(row_i <= col_i, 1.0, 0.0).astype(F32)
    lower = jnp.where(row_i >= col_i, 1.0, 0.0).astype(F32)
    for b in range(2):
        part = logp_v[:, b * BLOCK : (b + 1) * BLOCK]
        r_v[b] = dot_nn(part, upper, HIGH)
        rt_v[b * BLOCK : (b + 1) * BLOCK, :] = dot_nt(lower, part, HIGH)

    mix_v[...] = jnp.zeros_like(mix_v)
    lane_i = lax.broadcasted_iota(jnp.int32, (2 * BLOCK, N), 1)

    def column(h):
        return jnp.sum(jnp.where(lane_i == h, rt_v[...], 0.0), axis=1, keepdims=True)

    half = BLOCK // 2
    tri_a = lax.broadcasted_iota(jnp.int32, (half, BLOCK), 1) >= lax.broadcasted_iota(jnp.int32, (half, BLOCK), 0)
    tri_b = lax.broadcasted_iota(jnp.int32, (half, half), 1) >= lax.broadcasted_iota(jnp.int32, (half, half), 0)

    def decays(rt, rs):
        top = jnp.exp(jnp.where(tri_a, rs - rt[0:half], -jnp.inf))
        bottom = jnp.exp(jnp.where(tri_b, rs[:, half:] - rt[half:], -jnp.inf))
        return top, bottom

    def mix_pair(hp, carry):
        adds = [[None, None], [None, None]]
        for j in range(2):
            h = hp * 2 + j
            lanes = pl.ds(pl.multiple_of(h * N, N), N)
            col = column(h)
            for b in range(2):
                at = pl.ds(b * BLOCK, BLOCK)
                xb = x_v[at, lanes]
                db = dy_v[at, lanes]
                rt = col[b * BLOCK : (b + 1) * BLOCK]
                rs = r_v[b, pl.ds(h, 1), :]
                prod = dot_nt(xb, db)
                top, bottom = decays(rt, rs)
                top = top * prod[0:half]
                bottom = bottom * prod[half:, half:]
                adds[b][0] = top if j == 0 else adds[b][0] + top
                adds[b][1] = bottom if j == 0 else adds[b][1] + bottom
                closing = rt[BLOCK - 1 : BLOCK]
                erow_v[b, :, lanes] = jnp.broadcast_to(jnp.exp(closing), (8, N))
                xs_v[at, lanes] = (xb.astype(F32) * jnp.exp(closing - rt)).astype(BF16)
                ds_v[at, lanes] = (db.astype(F32) * jnp.exp(rt)).astype(BF16)
        for b in range(2):
            mix_v[b, 0:half, :] += adds[b][0]
            mix_v[b, half:, half:] += adds[b][1]
        return carry

    pairs = heads // 2

    def mix_group(first_pair, last_pair):
        for g in range(groups):
            if first_pair <= g * (pairs // groups) < last_pair:
                for copy in in_copies(g):
                    copy.wait()
        lax.fori_loop(first_pair, last_pair, mix_pair, 0)

    cuts = (0, pairs // 8, pairs // 4, pairs * 3 // 8, pairs)
    mix_group(cuts[0], cuts[1])
    wait_bytes(wl_v.at[0, 0, pl.ds(0, opts - 1)], recv_sem.at[0])
    for k in far_first:
        same(wl_v.at[chip, core, :], send_sem.at[2], blk_sem.at[k], yz(k)[1]).start()
    same(wl_v.at[chip, core, :], send_sem.at[3], recv_sem.at[3], partner).start()
    wait_bytes(rx_v.at[pl.ds(0, opts - 1)], recv_sem.at[13])
    old_sum = rx_v[0]
    for k in range(1, opts):
        old_sum = old_sum + rx_v[k]
    dlo_v[...] = old_sum
    dlo_v[0:1, :] = rt_v[BLOCK - 1 : BLOCK, :] + rt_v[2 * BLOCK - 1 : 2 * BLOCK, :]
    remote(dlo_v, dlp_v, send_sem.at[1], recv_sem.at[1], partner).start()
    mix_group(cuts[1], cuts[2])
    wait_bytes(wr_v.at[pl.ds(0, chips - 1), 0, 0], recv_sem.at[12])
    for k in range(1, opts):
        same(wr_v.at[:, core, opt], send_sem.at[15], half_sem.at[k], xp(k)[1]).start()
    same(wr_v.at[:, core, opt], send_sem.at[3], recv_sem.at[3], partner).start()
    mix_group(cuts[2], cuts[3])
    wait_bytes(dlp_v, recv_sem.at[1])
    dc_v[chip] = dlo_v[...] + dlp_v[...]
    for k in far_first:
        same(dc_v.at[chip], send_sem.at[4], recv_sem.at[4], yz(k)[1]).start()
    mix_group(cuts[3], cuts[4])
    for k in range(1, chips):
        block = wl_v.at[owner_before(k), core, :]
        wait_bytes(block, blk_sem.at[k])
        same(block, send_sem.at[3], recv_sem.at[3], partner).start()
    for k in range(1, opts):
        block = wr_v.at[:, core, (opt + opts - k) % opts]
        wait_bytes(block, half_sem.at[k])
        same(block, send_sem.at[3], recv_sem.at[3], partner).start()
    lay_copy.wait()
    wait_bytes(wl_v, recv_sem.at[3])

    proj = dot_nn(lay_v[...], jnp.concatenate([wl_v[...].reshape(dim, N), wr_v[...].reshape(dim, N)], axis=1)).astype(BF16)
    bc_v[...] = proj
    bct_v[...] = jnp.transpose(proj.astype(F32)).astype(BF16)
    for b in range(2):
        at = slice(b * BLOCK, (b + 1) * BLOCK)
        aff_v[b] = dot_nt(bc_v[at, 0:N], bc_v[at, N : 2 * N])

    def add_pair(way, k, carry):
        lanes = pl.ds(pl.multiple_of(owner_after(k) * 2 * N, 2 * N), 2 * N)
        if way == 0:
            first_blk = dot_nn(bct_v[0:N, 0:BLOCK], xs_v[0:BLOCK, lanes])
            second_blk = dot_nn(bct_v[0:N, BLOCK:], xs_v[BLOCK:, lanes])
            f0_v[:, lanes] = first_blk
            both = (erow_v[1, 0:1, lanes] * first_blk + second_blk).astype(BF16)
        else:
            first_blk = dot_nn(bct_v[N:, 0:BLOCK], ds_v[0:BLOCK, lanes])
            second_blk = dot_nn(bct_v[N:, BLOCK:], ds_v[BLOCK:, lanes])
            k1_v[:, lanes] = second_blk
            both = (first_blk + erow_v[0, 0:1, lanes] * second_blk).astype(BF16)
        for j in range(2):
            t_v[way, j, k] = both[:, j * N : (j + 1) * N]
        return carry

    lane_r = lax.broadcasted_iota(jnp.int32, (1, N), 1)

    def decay_of(ref, h):
        return jnp.exp(jnp.sum(jnp.where(lane_r == h, ref[0:1, :], 0.0), axis=1, keepdims=True))

    first = core == 0

    def combine(way, k, carry):
        h = 2 * owner_after(k) + core
        mine = decay_of(dlo_v, h)
        theirs = decay_of(dlp_v, h)
        one = jnp.ones_like(mine)
        own = t_v[way, core, k].astype(F32)
        other = pt_v[way, k].astype(F32)
        if way == 0:
            both = jnp.where(first, theirs, one) * own + jnp.where(first, one, mine) * other
        else:
            both = jnp.where(first, one, theirs) * own + jnp.where(first, mine, one) * other
        cb_v[way, k] = both.astype(BF16)
        return carry

    def piece(g, size):
        return chips - (g + 1) * size

    def combine_group(way, g):
        start = piece(g, per)
        at = pl.ds(start, per)
        wait_bytes(pt_v.at[way, at], d2d_sem.at[way, g])
        lax.fori_loop(start, start + per, functools.partial(combine, way), 0, unroll=True)
        for k in reversed(range(max(1, start), start + per)):
            remote(cb_v.at[way, k], rb_v.at[way, chip], send_sem.at[6], recv_sem.at[6 + way], yz(k)[1]).start()

    steps = [(way, g) for way in range(2) for g in range(parts)]
    for i, (way, g) in enumerate(steps):
        start = piece(g, per)
        at = pl.ds(start, per)
        lax.fori_loop(start, start + per, functools.partial(add_pair, way), 0, unroll=True)
        remote(t_v.at[way, 1 - core, at], pt_v.at[way, at], send_sem.at[5], d2d_sem.at[way, g], partner).start()
        if i >= 2:
            combine_group(*steps[i - 2])
    for i in range(len(steps) - 2, len(steps)):
        combine_group(*steps[i])
    for way in range(2):
        rb_v[way, chip] = cb_v[way, 0]

    lane_h = lax.broadcasted_iota(jnp.int32, (1, heads), 1)

    def inner_pair(hp, carry):
        for j in range(2):
            h = hp * 2 + j
            lanes = pl.ds(pl.multiple_of(h * N, N), N)
            col = column(h)
            gain = jnp.sum(jnp.where(lane_h == h, skip_ref[...], 0.0), axis=1, keepdims=True)
            for b in range(2):
                rt = col[b * BLOCK : (b + 1) * BLOCK]
                rs = r_v[b, pl.ds(h, 1), :]
                top, bottom = decays(rt, rs)
                top = (top * aff_v[b, 0:half, :]).astype(BF16)
                bottom = (bottom * aff_v[b, half:, half:]).astype(BF16)
                db = dy_v[pl.ds(b * BLOCK, BLOCK), lanes]
                low = db[half:]
                gi_v[pl.ds(b * BLOCK, half), lanes] = (dot_nn(top, db) + gain * db[0:half].astype(F32)).astype(BF16)
                gi_v[pl.ds(b * BLOCK + half, half), lanes] = (dot_nn(bottom, low) + gain * low.astype(F32)).astype(BF16)
        return carry

    lane_c = lax.broadcasted_iota(jnp.int32, (chips, N), 1)

    def scan_chips(way):
        wait_bytes(rb_v.at[way, pl.ds(0, chips - 1)], recv_sem.at[6 + way])
        chip_decay = jnp.exp(jnp.sum(jnp.where(lane_c == seq, dc_v[:, 0, :], 0.0), axis=1, keepdims=True))
        run = jnp.zeros((N, N), F32)
        for o in range(chips) if way == 0 else reversed(range(chips)):
            ob_v[way, o] = run.astype(BF16)
            run = chip_decay[o : o + 1] * run + rb_v[way, o].astype(F32)
        for k in far_first:
            other, dev = yz(k)
            remote(ob_v.at[way, other], ib_v.at[way, k], send_sem.at[7], entry_sem.at[way, k], dev).start()
        ib_v[way, 0] = ob_v[way, chip]

    lax.fori_loop(0, heads // 4, inner_pair, 0)
    wait_bytes(dc_v.at[pl.ds(0, chips - 1)], recv_sem.at[4])
    scan_chips(0)
    lax.fori_loop(heads // 4, heads // 2, inner_pair, 0)
    scan_chips(1)

    for b in range(2):
        at = slice(b * BLOCK, (b + 1) * BLOCK)
        mix = mix_v[b].astype(BF16)
        gbt_v[0:N, at] = dot_nt(bct_v[N:, at], mix)
        gbt_v[N:, at] = dot_nn(bct_v[0:N, at], mix)

    def entry(way, k, carry):
        h = 2 * owner_before(k) + core
        back = opposite(k)
        mine = decay_of(dlo_v, h)
        theirs = decay_of(dlp_v, h)
        one = jnp.ones_like(mine)
        nil = jnp.zeros_like(mine)
        came = ib_v[way, k].astype(F32)
        own = t_v[way, core, back].astype(F32)
        other = pt_v[way, back].astype(F32)
        if way == 0:
            here = jnp.where(first, one, theirs) * came + jnp.where(first, nil, one) * other
            there = jnp.where(first, mine, one) * came + jnp.where(first, one, nil) * own
        else:
            here = jnp.where(first, theirs, one) * came + jnp.where(first, one, nil) * other
            there = jnp.where(first, one, mine) * came + jnp.where(first, nil, one) * own
        fin_v[way, core, k] = here.astype(BF16)
        xb_v[way, k] = there.astype(BF16)
        return carry

    def finish_pair(way, k, carry):
        o = owner_before(k)
        lanes = pl.ds(pl.multiple_of(o * 2 * N, 2 * N), 2 * N)
        came = jnp.concatenate([fin_v[way, 0, k], fin_v[way, 1, k]], axis=1)
        if way == 0:
            later = (f0_v[:, lanes] + erow_v[0, 0:1, lanes] * came.astype(F32)).astype(BF16)
            for b, st in enumerate((came, later)):
                at = slice(b * BLOCK, (b + 1) * BLOCK)
                gbt_v[N:, at] += dot_nt(st, ds_v[at, lanes])
            return carry
        earlier = (k1_v[:, lanes] + erow_v[1, 0:1, lanes] * came.astype(F32)).astype(BF16)
        for b, gr in enumerate((earlier, came)):
            at = slice(b * BLOCK, (b + 1) * BLOCK)
            gbt_v[0:N, at] += dot_nt(gr, xs_v[at, lanes])
        return carry

    def outer_pair(k, carry):
        o = owner_before(k)
        lanes = pl.ds(pl.multiple_of(o * 2 * N, 2 * N), 2 * N)
        came = jnp.concatenate([fin_v[1, 0, k], fin_v[1, 1, k]], axis=1)
        earlier = (k1_v[:, lanes] + erow_v[1, 0:1, lanes] * came.astype(F32)).astype(BF16)
        cols = [column(2 * o), column(2 * o + 1)]
        for b, gr in enumerate((earlier, came)):
            at = slice(b * BLOCK, (b + 1) * BLOCK)
            outer = dot_nn(bc_v[at, 0:N], gr)
            for j in range(2):
                sub = pl.ds(pl.multiple_of((o * 2 + j) * N, N), N)
                rt = cols[j][at]
                shrink = jnp.exp(rt[BLOCK - 1 : BLOCK] - rt)
                gi_v[at, sub] = (gi_v[at, sub].astype(F32) + shrink * outer[:, j * N : (j + 1) * N]).astype(BF16)
        return carry

    def finish_group(way, g):
        start = piece(g, fine)
        wait_bytes(xb_v.at[way, pl.ds(start, fine)], fin_sem.at[way, g])
        lax.fori_loop(start, start + fine, functools.partial(finish_pair, way), 0, unroll=True)

    steps = [(way, g) for way in range(2) for g in range(fines)]
    behind = 3
    for i, (way, g) in enumerate(steps):
        start = piece(g, fine)
        at = pl.ds(start, fine)
        for k in reversed(range(max(1, start), start + fine)):
            wait_bytes(ib_v.at[way, k], entry_sem.at[way, k])
        lax.fori_loop(start, start + fine, functools.partial(entry, way), 0, unroll=True)
        remote(xb_v.at[way, at], fin_v.at[way, core, at], send_sem.at[8], fin_sem.at[way, g], partner).start()
        if i >= behind:
            finish_group(*steps[i - behind])
    for i in range(max(0, len(steps) - behind), len(steps)):
        finish_group(*steps[i])

    gbt_b = gbt_v[...].astype(BF16)

    def weight_pair(k, carry):
        lanes = pl.ds(pl.multiple_of(owner_after(k) * 2 * rblk, 2 * rblk), 2 * rblk)
        part = dot_nn(gbt_b, lay_v[:, lanes]).astype(BF16)
        wg_v[0, k] = part[:, 0:rblk]
        wg_v[1, k] = part[:, rblk:]
        return carry

    def chip_sum(k, carry):
        rss_v[k] = (wg_v[core, k].astype(F32) + rd_v[k].astype(F32)).astype(BF16)
        return carry

    cols = 2 * N
    main = cols * 3 // 4
    share = (cols - main) // opts

    def quarter(who):
        return pl.ds(pl.multiple_of(main + who * share, share), share)

    def sum_group(g):
        start = piece(g, fine)
        at = pl.ds(start, fine)
        wait_bytes(rd_v.at[at], rs_sem.at[g])
        lax.fori_loop(start, start + fine, chip_sum, 0, unroll=True)
        for k in reversed(range(max(1, start), start + fine)):
            top = pl.ds(0, main)
            remote(rss_v.at[k, top], rsr_v.at[k], send_sem.at[10], recv_sem.at[10], yz(k)[1]).start()
        if (g + 1) * 2 % fines == 0:
            half_at = pl.ds(start, chips // 2)
            for k in range(1, opts):
                other, dev = xp(k)
                remote(
                    rss_v.at[half_at, quarter(other)], bx_v.at[opt, half_at], send_sem.at[18], recv_sem.at[18], dev
                ).start()

    lag = 2
    for g in range(fines):
        start = piece(g, fine)
        at = pl.ds(start, fine)
        lax.fori_loop(start, start + fine, weight_pair, 0, unroll=True)
        remote(wg_v.at[1 - core, at], rd_v.at[at], send_sem.at[9], rs_sem.at[g], partner).start()
        if g >= lag:
            sum_group(g - lag)
    for g in range(max(0, fines - lag), fines):
        sum_group(g)
    rsr_v[0] = rss_v[0, 0:main]
    bx_v[opt] = rss_v[:, quarter(opt)]

    lax.fori_loop(0, chips // 2, outer_pair, 0)

    wait_bytes(bx_v.at[pl.ds(0, opts - 1)], recv_sem.at[18])
    part = bx_v[0].astype(F32)
    for k in range(1, opts):
        part = part + bx_v[k].astype(F32)
    by_v[...] = part.astype(BF16)
    for k in far_first:
        remote(by_v.at[k], bz_v.at[k], send_sem.at[19], recv_sem.at[19], yz(k)[1]).start()
    bz_v[0] = by_v[0]
    lax.fori_loop(chips // 2, chips, outer_pair, 0)

    wait_bytes(rsr_v.at[pl.ds(0, chips - 1)], recv_sem.at[10])
    acc = rsr_v[0].astype(F32)
    for k in range(1, chips):
        acc = acc + rsr_v[k].astype(F32)
    xg_v[opt] = acc.astype(BF16)
    for k in range(1, opts):
        same(xg_v.at[opt], send_sem.at[11], recv_sem.at[11], xp(k)[1]).start()

    wait_bytes(bz_v.at[pl.ds(0, chips - 1)], recv_sem.at[19])
    acc = bz_v[0].astype(F32)
    for k in range(1, chips):
        acc = acc + bz_v[k].astype(F32)
    bw_v[opt] = acc
    for k in range(1, opts):
        same(bw_v.at[opt], send_sem.at[20], recv_sem.at[20], xp(k)[1]).start()

    wait_bytes(mc_v.at[pl.ds(0, opts - 1)], recv_sem.at[14])
    wait_bytes(xg_v.at[pl.ds(0, opts - 1)], recv_sem.at[11])
    acc = xg_v[0].astype(F32)
    for k in range(1, opts):
        acc = acc + xg_v[k].astype(F32)
    wait_bytes(bw_v.at[pl.ds(0, opts - 1)], recv_sem.at[20])
    grad = jnp.transpose(jnp.concatenate([acc] + [bw_v[k] for k in range(opts)], axis=0))
    gt_v[...] = grad

    def over_all(buf, row, base, combine_fn):
        buf[seq, 0:1] = row
        for k in range(1, seqs):
            same(buf.at[seq, 0:1], send_sem.at[base], recv_sem.at[base], ((seq + k) % seqs, opt)).start()
        wait_bytes(buf.at[pl.ds(0, seqs - 1), 0:1], recv_sem.at[base])
        value = buf[0, 0:1]
        for k in range(1, seqs):
            value = combine_fn(value, buf[k, 0:1])
        return value

    col_raw = over_all(s_v, jnp.sum(grad * grad, axis=0, keepdims=True), 16, jnp.add)
    raw_total = jnp.sum(col_raw, axis=1, keepdims=True)
    factor = jnp.minimum(1.0, clip_norm / jnp.sqrt(raw_total + norm_floor))

    def moment_of(code, part):
        return beta_one * code.astype(F32) * mscale_ref[...] + (1.0 - beta_one) * (part * factor)

    top = jnp.zeros((1, 2 * N), F32)
    for k in range(opts):
        part = moment_of(mc_v[k], gt_v[k * rows : (k + 1) * rows])
        top = jnp.maximum(top, jnp.max(jnp.abs(part), axis=0, keepdims=True))
    peak = over_all(m_v, top, 17, jnp.maximum)

    own = gt_v[pl.ds(pl.multiple_of(opt * rows, rows), rows), :]
    scaled = own * factor
    moment = moment_of(mc_v[opt], own)
    squares = scaled * scaled
    old_total = jnp.sum(dc_v[:, 1, 0:1], axis=0, keepdims=True)
    col_next = beta_two * colstat_ref[...] + (1.0 - beta_two) * (factor * factor * col_raw / dim + tiny_square)
    eye = lax.broadcasted_iota(jnp.int32, (rows, rows), 0) == lax.broadcasted_iota(jnp.int32, (rows, rows), 1)
    old_col = jnp.sum(jnp.where(eye, jnp.broadcast_to(old_row, (rows, rows)), 0.0), axis=1, keepdims=True)
    row_next = beta_two * old_col + (1.0 - beta_two) * (
        jnp.sum(squares, axis=1, keepdims=True) / (2 * N) + tiny_square
    )
    row_mean = (
        beta_two * old_total + (1.0 - beta_two) * (factor * factor * raw_total / (2 * N) + dim * tiny_square)
    ) / dim
    second = row_next * col_next / row_mean
    upd_ref[...] = moment / (jnp.sqrt(second) + adam_floor) + weight_decay * w_ref[...]
    scale_next = peak + peak_floor
    scaleo_ref[...] = scale_next
    codeo_ref[...] = (moment / scale_next).astype(BF16)
    colo_ref[...] = col_next
    rowo_ref[...] = jnp.sum(jnp.where(eye, jnp.broadcast_to(row_next, (rows, rows)), 0.0), axis=0, keepdims=True)

    wait_bytes(wl_v.at[0, 0, pl.ds(0, opts - 1)], send_sem.at[0])
    wait_bytes(dlo_v, send_sem.at[1])
    wait_bytes(wl_v.at[pl.ds(0, chips - 1), 0, :], send_sem.at[2])
    wait_bytes(wl_v, send_sem.at[3])
    wait_bytes(dc_v.at[pl.ds(0, chips - 1)], send_sem.at[4])
    wait_bytes(pt_v, send_sem.at[5])
    wait_bytes(cb_v.at[:, pl.ds(0, chips - 1)], send_sem.at[6])
    wait_bytes(ob_v.at[:, pl.ds(0, chips - 1)], send_sem.at[7])
    wait_bytes(xb_v, send_sem.at[8])
    wait_bytes(rd_v, send_sem.at[9])
    wait_bytes(rsr_v.at[pl.ds(0, chips - 1)], send_sem.at[10])
    wait_bytes(xg_v.at[pl.ds(0, opts - 1)], send_sem.at[11])
    wait_bytes(wr_v.at[pl.ds(0, chips - 1), 0, 0], send_sem.at[12])
    wait_bytes(rx_v.at[pl.ds(0, opts - 1)], send_sem.at[13])
    wait_bytes(mc_v.at[pl.ds(0, opts - 1)], send_sem.at[14])
    wait_bytes(wr_v.at[:, 0, pl.ds(0, opts - 1)], send_sem.at[15])
    wait_bytes(bx_v.at[pl.ds(0, opts - 1)], send_sem.at[18])
    wait_bytes(by_v.at[pl.ds(0, chips - 1)], send_sem.at[19])
    wait_bytes(bw_v.at[pl.ds(0, opts - 1)], send_sem.at[20])
    for base, buf in ((16, s_v), (17, m_v)):
        wait_bytes(buf.at[pl.ds(0, seqs - 1), 0:1], send_sem.at[base])


def copy_out(*refs):
    sem = refs[-1]
    copies = []
    gi_ref, gi_out = refs[0], refs[6]
    pieces = 4
    size = gi_ref.shape[0] // pieces
    for k in range(pieces):
        at = pl.ds(k * size, size)
        copies.append(pltpu.make_async_copy(gi_ref.at[at], gi_out.at[at], sem.at[k]))
    for k in range(1, 6):
        copies.append(pltpu.make_async_copy(refs[k], refs[6 + k], sem.at[pieces + k - 1]))
    for copy in copies:
        copy.start()
    for copy in copies:
        copy.wait()


def per_device(
    seqs, opts, layer_in, ssm_input, grad_out, log_decay, skip_gain, w_bc, m_code, m_scale, row_stat, col_stat
):
    heads = skip_gain.shape[0]
    tokens, width = ssm_input.shape[1:]
    dim = layer_in.shape[2]
    rows = w_bc.shape[0]
    chips = seqs // 2
    rblk = rows * opts
    vm = pl.BlockSpec(memory_space=pltpu.VMEM)
    hbm = pl.BlockSpec(memory_space=pl.ANY)
    state = (2, chips, N, N)
    main = 2 * N * 3 // 4
    share = (2 * N - main) // opts
    scratch = [
        pltpu.VMEM((tokens, width), BF16),
        pltpu.VMEM((tokens, width), BF16),
        pltpu.VMEM((tokens, dim), BF16),
        pltpu.VMEM((tokens, width), BF16),
        pltpu.VMEM((tokens, width), BF16),
        pltpu.VMEM((chips, 2, opts, rows, N), BF16),
        pltpu.VMEM((chips, 2, opts, rows, N), BF16),
        pltpu.VMEM((N, tokens), F32),
        pltpu.VMEM((1, heads), F32),
        pltpu.VMEM((rows, 2 * N), F32),
        pltpu.VMEM((1, 2 * N), F32),
        pltpu.VMEM((1, rows), F32),
        pltpu.VMEM((1, 2 * N), F32),
        pltpu.VMEM((2, N, BLOCK), F32),
        pltpu.VMEM((tokens, N), F32),
        pltpu.VMEM((2, 8, width), F32),
        pltpu.VMEM((2, BLOCK, BLOCK), F32),
        pltpu.VMEM((2, BLOCK, BLOCK), F32),
        pltpu.VMEM((tokens, 2 * N), BF16),
        pltpu.VMEM((2 * N, tokens), BF16),
        pltpu.VMEM((N, width), F32),
        pltpu.VMEM((N, width), F32),
        pltpu.VMEM((2, 2, chips, N, N), BF16),
        pltpu.VMEM(state, BF16),
        pltpu.VMEM(state, BF16),
        pltpu.VMEM(state, BF16),
        pltpu.VMEM(state, BF16),
        pltpu.VMEM(state, BF16),
        pltpu.VMEM(state, BF16),
        pltpu.VMEM((2, 2, chips, N, N), BF16),
        pltpu.VMEM((2 * N, tokens), F32),
        pltpu.VMEM((2, chips, 2 * N, rblk), BF16),
        pltpu.VMEM((chips, 2 * N, rblk), BF16),
        pltpu.VMEM((chips, 2 * N, rblk), BF16),
        pltpu.VMEM((chips, main, rblk), BF16),
        pltpu.VMEM((opts, chips, share, rblk), BF16),
        pltpu.VMEM((chips, share, rblk), BF16),
        pltpu.VMEM((chips, share, rblk), BF16),
        pltpu.VMEM((opts, share, rblk), F32),
        pltpu.VMEM((opts, main, rblk), BF16),
        pltpu.VMEM((rblk, 2 * N), F32),
        pltpu.VMEM((opts, rows, 2 * N), BF16),
        pltpu.VMEM((opts, 8, N), F32),
        pltpu.VMEM((8, N), F32),
        pltpu.VMEM((8, N), F32),
        pltpu.VMEM((chips, 8, N), F32),
        pltpu.VMEM((seqs, 8, 2 * N), F32),
        pltpu.VMEM((seqs, 8, 2 * N), F32),
        pltpu.SemaphoreType.DMA((9,)),
        pltpu.SemaphoreType.DMA((7,)),
        pltpu.SemaphoreType.DMA((21,)),
        pltpu.SemaphoreType.DMA((21,)),
        pltpu.SemaphoreType.DMA((chips,)),
        pltpu.SemaphoreType.DMA((opts,)),
        pltpu.SemaphoreType.DMA((2, chips)),
        pltpu.SemaphoreType.DMA((2, 4)),
        pltpu.SemaphoreType.DMA((2, min(8, chips))),
        pltpu.SemaphoreType.DMA((min(8, chips),)),
    ]
    shapes = (
        jax.ShapeDtypeStruct((tokens, width), BF16),
        jax.ShapeDtypeStruct((rows, 2 * N), F32),
        jax.ShapeDtypeStruct((rows, 2 * N), BF16),
        jax.ShapeDtypeStruct((1, 2 * N), F32),
        jax.ShapeDtypeStruct((1, rows), F32),
        jax.ShapeDtypeStruct((1, 2 * N), F32),
    )
    out = pl.pallas_call(
        functools.partial(kernel, seqs, opts),
        out_shape=tuple(pltpu.VMEM(a.shape, a.dtype) for a in shapes),
        in_specs=[hbm] * 10,
        out_specs=(vm, vm, vm, vm, vm, vm),
        scratch_shapes=scratch,
        compiler_params=pltpu.CompilerParams(
            collective_id=0, has_side_effects=True, vmem_limit_bytes=60_000_000
        ),
    )(
        ssm_input[0],
        grad_out[0],
        layer_in[0],
        log_decay[0],
        skip_gain.reshape(1, heads),
        w_bc,
        m_code,
        m_scale.reshape(1, 2 * N),
        row_stat.reshape(1, rows),
        col_stat.reshape(1, 2 * N),
    )
    grad_input, update, code_next, scale_next, row_next, col_next = pl.pallas_call(
        copy_out,
        out_shape=shapes,
        in_specs=[vm] * 6,
        out_specs=(hbm,) * 6,
        scratch_shapes=[pltpu.SemaphoreType.DMA((9,))],
        compiler_params=pltpu.CompilerParams(vmem_limit_bytes=4_000_000),
    )(*[pltpu.with_memory_space_constraint(a, pltpu.VMEM) for a in out])
    return (
        grad_input[None],
        update,
        code_next,
        scale_next.reshape(2 * N),
        row_next.reshape(rows),
        col_next.reshape(2 * N),
    )


def solution(mesh):
    both = ("seq", "opt")
    return jax.shard_map(
        functools.partial(per_device, mesh.shape["seq"], mesh.shape["opt"]),
        mesh=mesh,
        in_specs=(
            P("opt", "seq", None),
            P("opt", "seq", None),
            P("opt", "seq", None),
            P("opt", None, "seq"),
            P(),
            P(both, None),
            P(both, None),
            P(),
            P(both),
            P(),
        ),
        out_specs=(P("opt", "seq", None), P(both, None), P(both, None), P(), P(both), P()),
        check_vma=False,
    )
```

```python
import functools
import math

import jax
import jax.numpy as jnp
from jax import lax
from jax.experimental import pallas as pl
from jax.experimental.pallas import tpu as pltpu
from jax.sharding import PartitionSpec as P

MESH = pl.DeviceIdType.MESH
BLOCK = 256
N = 128
F32 = jnp.float32
BF16 = jnp.bfloat16
HIGH = lax.Precision.HIGHEST

beta_one = 0.9
beta_two = 0.95
weight_decay = 0.1
clip_norm = 1.0
tiny_square = 1e-30
adam_floor = 1e-08
peak_floor = 1e-06
norm_floor = 1e-06


def dot_nn(a, b, precision=None):
    return lax.dot_general(a, b, (((1,), (0,)), ((), ())), preferred_element_type=F32, precision=precision)


def dot_nt(a, b, precision=None):
    return lax.dot_general(a, b, (((1,), (1,)), ((), ())), preferred_element_type=F32, precision=precision)


def kernel(
    seqs,
    opts,
    x_hbm,
    dy_hbm,
    lay_hbm,
    logs_hbm,
    skip_hbm,
    w_hbm,
    code_hbm,
    mscale_hbm,
    rowstat_hbm,
    colstat_hbm,
    gi_v,
    upd_ref,
    codeo_ref,
    scaleo_ref,
    rowo_ref,
    colo_ref,
    x_v,
    dy_v,
    lay_v,
    xs_v,
    ds_v,
    wl_v,
    wr_v,
    logp_v,
    skip_ref,
    w_ref,
    mscale_ref,
    rowstat_ref,
    colstat_ref,
    r_v,
    rt_v,
    erow_v,
    mix_v,
    aff_v,
    proj_v,
    bc_v,
    bct_v,
    f0_v,
    k1_v,
    t_v,
    pt_v,
    cb_v,
    rb_v,
    ob_v,
    ib_v,
    xb_v,
    fin_v,
    gbt_v,
    gbt_b,
    wg_v,
    rd_v,
    rss_v,
    rsr_v,
    bx_v,
    by_v,
    bz_v,
    bw_v,
    xg_v,
    gt_v,
    mc_v,
    rx_v,
    dlo_v,
    dlp_v,
    dc_v,
    s_v,
    m_v,
    in_sem,
    small_sem,
    send_sem,
    recv_sem,
    blk_sem,
    half_sem,
    entry_sem,
    d2d_sem,
    fin_sem,
    rs_sem,
):
    heads = skip_ref.shape[1]
    chips = seqs // 2
    rows = w_ref.shape[0]
    rblk = rows * opts
    width = x_hbm.shape[1]
    dim = lay_hbm.shape[1]
    groups = 4
    lanes_g = width // groups
    fines = min(8, chips)
    fine = chips // fines
    parts = 4
    per = chips // parts

    seq = lax.axis_index("seq")
    opt = lax.axis_index("opt")
    chip = seq // 2
    core = seq % 2
    mate = chip * 2 + (1 - core)
    partner = (mate, opt)

    side = math.isqrt(chips)

    def step_of(i):
        return (i * (i + 1) // 2) % side

    def owner_after(e):
        zs = (chip // side + step_of(e // side)) % side
        ys = (chip % side + step_of(e % side)) % side
        return zs * side + ys

    def owner_before(e):
        zs = (chip // side + side - step_of(e // side)) % side
        ys = (chip % side + side - step_of(e % side)) % side
        return zs * side + ys

    def flip(i):
        return 2 * (i % 2) + i // 2 if side == 4 else i

    def opposite(e):
        return flip(e // side) * side + flip(e % side)

    far_first = tuple(range(chips - 1, 0, -1))

    def yz(e):
        other = owner_after(e)
        return other, (other * 2 + core, opt)

    def xp(k):
        other = (opt + k) % opts
        return other, (seq, other)

    def remote(src, dst, s_sem, r_sem, dev):
        return pltpu.make_async_remote_copy(
            src_ref=src, dst_ref=dst, send_sem=s_sem, recv_sem=r_sem, device_id=dev, device_id_type=MESH
        )

    def wait_bytes(ref, sem):
        pltpu.make_async_copy(ref, ref, sem).wait()

    def in_copies(g):
        lanes = pl.ds(g * lanes_g, lanes_g)
        return (
            pltpu.make_async_copy(x_hbm.at[:, lanes], x_v.at[:, lanes], in_sem.at[2 * g]),
            pltpu.make_async_copy(dy_hbm.at[:, lanes], dy_v.at[:, lanes], in_sem.at[2 * g + 1]),
        )

    lay_copy = pltpu.make_async_copy(lay_hbm, lay_v, in_sem.at[2 * groups])

    def small(source, target, k):
        return pltpu.make_async_copy(source, target, small_sem.at[k])

    smalls = [
        small(w_hbm, w_ref, 0),
        small(rowstat_hbm, rowstat_ref, 1),
        small(code_hbm, mc_v.at[opt], 2),
        small(logs_hbm, logp_v.at[pl.ds(0, heads)], 3),
        small(skip_hbm, skip_ref, 4),
        small(mscale_hbm, mscale_ref, 5),
        small(colstat_hbm, colstat_ref, 6),
    ]
    barrier = pltpu.get_barrier_semaphore()
    for k in reversed(range(1, chips)):
        for who in range(2):
            pl.semaphore_signal(barrier, inc=1, device_id=(owner_after(k) * 2 + who, opt), device_id_type=MESH)
    pl.semaphore_signal(barrier, inc=1, device_id=partner, device_id_type=MESH)
    for k in range(1, opts):
        pl.semaphore_signal(barrier, inc=1, device_id=xp(k)[1], device_id_type=MESH)
    for copy in smalls:
        copy.start()
    if heads < N:
        logp_v[heads:, :] = jnp.zeros((N - heads, logp_v.shape[1]), F32)
    for copy in smalls:
        copy.wait()
    for g in range(groups):
        for copy in in_copies(g):
            copy.start()
    lay_copy.start()

    wl_v[chip, core, opt] = w_ref[:, 0:N].astype(BF16)
    wr_v[chip, core, opt] = w_ref[:, N:].astype(BF16)
    old_row = rowstat_ref[...]
    rx_v[opt] = jnp.broadcast_to(jnp.sum(old_row, axis=1, keepdims=True), (8, N))


    def same(ref, s_sem, r_sem, dev):
        return remote(ref, ref, s_sem, r_sem, dev)

    pl.semaphore_wait(barrier, seqs - 1 + opts - 1)
    for k in range(1, opts):
        same(wl_v.at[chip, core, opt], send_sem.at[0], recv_sem.at[0], xp(k)[1]).start()
    for k in far_first:
        same(wr_v.at[chip, core, opt], send_sem.at[12], recv_sem.at[12], yz(k)[1]).start()
    for k in range(1, opts):
        same(rx_v.at[opt], send_sem.at[13], recv_sem.at[13], xp(k)[1]).start()
        same(mc_v.at[opt], send_sem.at[14], recv_sem.at[14], xp(k)[1]).start()

    row_i = lax.broadcasted_iota(jnp.int32, (BLOCK, BLOCK), 0)
    col_i = lax.broadcasted_iota(jnp.int32, (BLOCK, BLOCK), 1)
    upper = jnp.where(row_i <= col_i, 1.0, 0.0).astype(F32)
    lower = jnp.where(row_i >= col_i, 1.0, 0.0).astype(F32)
    for b in range(2):
        part = logp_v[:, b * BLOCK : (b + 1) * BLOCK]
        r_v[b] = dot_nn(part, upper, HIGH)
        rt_v[b * BLOCK : (b + 1) * BLOCK, :] = dot_nt(lower, part, HIGH)

    mix_v[...] = jnp.zeros_like(mix_v)
    lane_i = lax.broadcasted_iota(jnp.int32, (2 * BLOCK, N), 1)

    def column(h):
        return jnp.sum(jnp.where(lane_i == h, rt_v[...], 0.0), axis=1, keepdims=True)

    half = BLOCK // 2
    tri_a = lax.broadcasted_iota(jnp.int32, (half, BLOCK), 1) >= lax.broadcasted_iota(jnp.int32, (half, BLOCK), 0)
    tri_b = lax.broadcasted_iota(jnp.int32, (half, half), 1) >= lax.broadcasted_iota(jnp.int32, (half, half), 0)

    def decays(rt, rs):
        top = jnp.exp(jnp.where(tri_a, rs - rt[0:half], -jnp.inf))
        bottom = jnp.exp(jnp.where(tri_b, rs[:, half:] - rt[half:], -jnp.inf))
        return top, bottom

    def mix_pair(products, scales, hp, carry):
        adds = [[None, None], [None, None]]
        for j in range(2):
            h = hp * 2 + j
            lanes = pl.ds(pl.multiple_of(h * N, N), N)
            col = column(h)
            for b in range(2):
                at = pl.ds(b * BLOCK, BLOCK)
                xb = x_v[at, lanes]
                db = dy_v[at, lanes]
                rt = col[b * BLOCK : (b + 1) * BLOCK]
                if products:
                    prod = dot_nt(xb, db)
                    top, bottom = decays(rt, r_v[b, pl.ds(h, 1), :])
                    top = top * prod[0:half]
                    bottom = bottom * prod[half:, half:]
                    adds[b][0] = top if j == 0 else adds[b][0] + top
                    adds[b][1] = bottom if j == 0 else adds[b][1] + bottom
                if scales:
                    closing = rt[BLOCK - 1 : BLOCK]
                    erow_v[b, :, lanes] = jnp.broadcast_to(jnp.exp(closing), (8, N))
                    xs_v[at, lanes] = (xb.astype(F32) * jnp.exp(closing - rt)).astype(BF16)
                    ds_v[at, lanes] = (db.astype(F32) * jnp.exp(rt)).astype(BF16)
        if products:
            for b in range(2):
                mix_v[b, 0:half, :] += adds[b][0]
                mix_v[b, half:, half:] += adds[b][1]
        return carry

    pairs = heads // 2

    def mix_group(first_part, last_part, products=True):
        first_pair, last_pair = (pairs * part // 16 for part in (first_part, last_part))
        for g in range(groups):
            if first_pair <= g * (pairs // groups) < last_pair:
                for copy in in_copies(g):
                    copy.wait()
        lax.fori_loop(first_pair, last_pair, functools.partial(mix_pair, products, True), 0)

    def share_left(some):
        for k in some:
            block = wl_v.at[owner_before(k), core]
            wait_bytes(block, blk_sem.at[k])
            same(block, send_sem.at[3], recv_sem.at[3], partner).start()

    mix_group(0, 2)
    wait_bytes(wl_v.at[0, 0, pl.ds(0, opts - 1)], recv_sem.at[0])
    for k in far_first:
        same(wl_v.at[chip, core], send_sem.at[2], blk_sem.at[k], yz(k)[1]).start()
    same(wl_v.at[chip, core], send_sem.at[3], recv_sem.at[3], partner).start()
    wait_bytes(rx_v.at[pl.ds(0, opts - 1)], recv_sem.at[13])
    old_sum = rx_v[0]
    for k in range(1, opts):
        old_sum = old_sum + rx_v[k]
    dlo_v[...] = old_sum
    dlo_v[0:1, :] = rt_v[BLOCK - 1 : BLOCK, :] + rt_v[2 * BLOCK - 1 : 2 * BLOCK, :]
    remote(dlo_v, dlp_v, send_sem.at[1], recv_sem.at[1], partner).start()
    mix_group(2, 3)
    wait_bytes(wr_v.at[pl.ds(0, chips - 1), 0, 0], recv_sem.at[12])
    for k in range(1, opts):
        same(wr_v.at[:, core, opt], send_sem.at[15], half_sem.at[k], xp(k)[1]).start()
    same(wr_v.at[:, core, opt], send_sem.at[3], recv_sem.at[3], partner).start()
    mix_group(3, 5)
    wait_bytes(dlp_v, recv_sem.at[1])
    dc_v[chip] = dlo_v[...] + dlp_v[...]
    for k in far_first:
        same(dc_v.at[chip], send_sem.at[4], recv_sem.at[4], yz(k)[1]).start()
    mix_group(5, 9)
    share_left(far_first[: chips // 2])
    mix_group(9, 10)
    mix_group(10, 13, products=False)
    share_left(far_first[chips // 2 :])
    mix_group(13, 16, products=False)
    for k in range(1, opts):
        block = wr_v.at[:, core, (opt + opts - k) % opts]
        wait_bytes(block, half_sem.at[k])
        same(block, send_sem.at[3], recv_sem.at[3], partner).start()
    lay_copy.wait()

    def proj_half(who):
        rows_in = jnp.concatenate(
            [lay_v[:, pl.ds(pl.multiple_of((2 * o + who) * rblk, rblk), rblk)] for o in range(chips)], axis=1
        )
        weights = [ref[:, who].reshape(chips * rblk, N) for ref in (wl_v, wr_v)]
        return dot_nn(rows_in, jnp.concatenate(weights, axis=1))

    proj_v[...] = proj_half(core)
    wait_bytes(wl_v, recv_sem.at[3])
    proj = (proj_v[...] + proj_half(1 - core)).astype(BF16)
    bc_v[...] = proj
    bct_v[...] = jnp.transpose(proj.astype(F32)).astype(BF16)
    for b in range(2):
        at = slice(b * BLOCK, (b + 1) * BLOCK)
        aff_v[b] = dot_nt(bc_v[at, 0:N], bc_v[at, N : 2 * N])

    def add_pair(way, k, carry):
        lanes = pl.ds(pl.multiple_of(owner_after(k) * 2 * N, 2 * N), 2 * N)
        if way == 0:
            first_blk = dot_nn(bct_v[0:N, 0:BLOCK], xs_v[0:BLOCK, lanes])
            second_blk = dot_nn(bct_v[0:N, BLOCK:], xs_v[BLOCK:, lanes])
            f0_v[:, lanes] = first_blk
            both = (erow_v[1, 0:1, lanes] * first_blk + second_blk).astype(BF16)
        else:
            first_blk = dot_nn(bct_v[N:, 0:BLOCK], ds_v[0:BLOCK, lanes])
            second_blk = dot_nn(bct_v[N:, BLOCK:], ds_v[BLOCK:, lanes])
            k1_v[:, lanes] = second_blk
            both = (first_blk + erow_v[0, 0:1, lanes] * second_blk).astype(BF16)
        for j in range(2):
            t_v[way, j, k] = both[:, j * N : (j + 1) * N]
        return carry

    lane_r = lax.broadcasted_iota(jnp.int32, (1, N), 1)

    def decay_of(ref, h):
        return jnp.exp(jnp.sum(jnp.where(lane_r == h, ref[0:1, :], 0.0), axis=1, keepdims=True))

    first = core == 0

    def combine(way, k, carry):
        h = 2 * owner_after(k) + core
        mine = decay_of(dlo_v, h)
        theirs = decay_of(dlp_v, h)
        one = jnp.ones_like(mine)
        own = t_v[way, core, k].astype(F32)
        other = pt_v[way, k].astype(F32)
        if way == 0:
            both = jnp.where(first, theirs, one) * own + jnp.where(first, one, mine) * other
        else:
            both = jnp.where(first, one, theirs) * own + jnp.where(first, mine, one) * other
        cb_v[way, k] = both.astype(BF16)
        return carry

    def piece(g, size):
        return chips - (g + 1) * size

    def combine_group(way, g):
        start = piece(g, per)
        at = pl.ds(start, per)
        wait_bytes(pt_v.at[way, at], d2d_sem.at[way, g])
        lax.fori_loop(start, start + per, functools.partial(combine, way), 0, unroll=True)
        for k in reversed(range(max(1, start), start + per)):
            remote(cb_v.at[way, k], rb_v.at[way, chip], send_sem.at[6], recv_sem.at[6 + way], yz(k)[1]).start()

    steps = [(way, g) for way in range(2) for g in range(parts)]
    for i, (way, g) in enumerate(steps):
        start = piece(g, per)
        at = pl.ds(start, per)
        lax.fori_loop(start, start + per, functools.partial(add_pair, way), 0, unroll=True)
        remote(t_v.at[way, 1 - core, at], pt_v.at[way, at], send_sem.at[5], d2d_sem.at[way, g], partner).start()
        if i >= 2:
            combine_group(*steps[i - 2])
    for i in range(len(steps) - 2, len(steps)):
        combine_group(*steps[i])
    for way in range(2):
        rb_v[way, chip] = cb_v[way, 0]

    lane_h = lax.broadcasted_iota(jnp.int32, (1, heads), 1)

    def inner_pair(hp, carry):
        for j in range(2):
            h = hp * 2 + j
            lanes = pl.ds(pl.multiple_of(h * N, N), N)
            col = column(h)
            gain = jnp.sum(jnp.where(lane_h == h, skip_ref[...], 0.0), axis=1, keepdims=True)
            for b in range(2):
                rt = col[b * BLOCK : (b + 1) * BLOCK]
                rs = r_v[b, pl.ds(h, 1), :]
                top, bottom = decays(rt, rs)
                top = (top * aff_v[b, 0:half, :]).astype(BF16)
                bottom = (bottom * aff_v[b, half:, half:]).astype(BF16)
                db = dy_v[pl.ds(b * BLOCK, BLOCK), lanes]
                low = db[half:]
                gi_v[pl.ds(b * BLOCK, half), lanes] = (dot_nn(top, db) + gain * db[0:half].astype(F32)).astype(BF16)
                gi_v[pl.ds(b * BLOCK + half, half), lanes] = (dot_nn(bottom, low) + gain * low.astype(F32)).astype(BF16)
        return carry

    lane_c = lax.broadcasted_iota(jnp.int32, (chips, N), 1)

    def scan_chips(way):
        wait_bytes(rb_v.at[way, pl.ds(0, chips - 1)], recv_sem.at[6 + way])
        chip_decay = jnp.exp(jnp.sum(jnp.where(lane_c == seq, dc_v[:, 0, :], 0.0), axis=1, keepdims=True))
        run = jnp.zeros((N, N), F32)
        for o in range(chips) if way == 0 else reversed(range(chips)):
            ob_v[way, o] = run.astype(BF16)
            run = chip_decay[o : o + 1] * run + rb_v[way, o].astype(F32)
        for k in far_first:
            other, dev = yz(k)
            remote(ob_v.at[way, other], ib_v.at[way, k], send_sem.at[7], entry_sem.at[way, k], dev).start()
        ib_v[way, 0] = ob_v[way, chip]

    lax.fori_loop(0, heads // 4, inner_pair, 0)
    lax.fori_loop(pairs * 10 // 16, pairs, functools.partial(mix_pair, True, False), 0)
    wait_bytes(dc_v.at[pl.ds(0, chips - 1)], recv_sem.at[4])
    scan_chips(0)
    lax.fori_loop(heads // 4, heads // 2, inner_pair, 0)
    scan_chips(1)

    for b in range(2):
        at = slice(b * BLOCK, (b + 1) * BLOCK)
        mix = mix_v[b].astype(BF16)
        gbt_v[0:N, at] = dot_nt(bct_v[N:, at], mix)
        gbt_v[N:, at] = dot_nn(bct_v[0:N, at], mix)

    def entry(way, k, carry):
        h = 2 * owner_before(k) + core
        back = opposite(k)
        mine = decay_of(dlo_v, h)
        theirs = decay_of(dlp_v, h)
        one = jnp.ones_like(mine)
        nil = jnp.zeros_like(mine)
        came = ib_v[way, k].astype(F32)
        own = t_v[way, core, back].astype(F32)
        other = pt_v[way, back].astype(F32)
        if way == 0:
            here = jnp.where(first, one, theirs) * came + jnp.where(first, nil, one) * other
            there = jnp.where(first, mine, one) * came + jnp.where(first, one, nil) * own
        else:
            here = jnp.where(first, theirs, one) * came + jnp.where(first, one, nil) * other
            there = jnp.where(first, one, mine) * came + jnp.where(first, nil, one) * own
        fin_v[way, core, k] = here.astype(BF16)
        xb_v[way, k] = there.astype(BF16)
        return carry

    def finish_pair(way, k, carry):
        o = owner_before(k)
        lanes = pl.ds(pl.multiple_of(o * 2 * N, 2 * N), 2 * N)
        came = jnp.concatenate([fin_v[way, 0, k], fin_v[way, 1, k]], axis=1)
        if way == 0:
            later = (f0_v[:, lanes] + erow_v[0, 0:1, lanes] * came.astype(F32)).astype(BF16)
            for b, st in enumerate((came, later)):
                at = slice(b * BLOCK, (b + 1) * BLOCK)
                gbt_v[N:, at] += dot_nt(st, ds_v[at, lanes])
            return carry
        earlier = (k1_v[:, lanes] + erow_v[1, 0:1, lanes] * came.astype(F32)).astype(BF16)
        for b, gr in enumerate((earlier, came)):
            at = slice(b * BLOCK, (b + 1) * BLOCK)
            gbt_v[0:N, at] += dot_nt(gr, xs_v[at, lanes])
        return carry

    def outer_pair(k, carry):
        o = owner_before(k)
        lanes = pl.ds(pl.multiple_of(o * 2 * N, 2 * N), 2 * N)
        came = jnp.concatenate([fin_v[1, 0, k], fin_v[1, 1, k]], axis=1)
        earlier = (k1_v[:, lanes] + erow_v[1, 0:1, lanes] * came.astype(F32)).astype(BF16)
        cols = [column(2 * o), column(2 * o + 1)]
        for b, gr in enumerate((earlier, came)):
            at = slice(b * BLOCK, (b + 1) * BLOCK)
            outer = dot_nn(bc_v[at, 0:N], gr)
            for j in range(2):
                sub = pl.ds(pl.multiple_of((o * 2 + j) * N, N), N)
                rt = cols[j][at]
                shrink = jnp.exp(rt[BLOCK - 1 : BLOCK] - rt)
                gi_v[at, sub] = (gi_v[at, sub].astype(F32) + shrink * outer[:, j * N : (j + 1) * N]).astype(BF16)
        return carry

    def finish_group(way, g):
        start = piece(g, fine)
        wait_bytes(xb_v.at[way, pl.ds(start, fine)], fin_sem.at[way, g])
        lax.fori_loop(start, start + fine, functools.partial(finish_pair, way), 0, unroll=True)

    behind = 3

    def enter_group(way, g):
        start = piece(g, fine)
        at = pl.ds(start, fine)
        for k in reversed(range(max(1, start), start + fine)):
            wait_bytes(ib_v.at[way, k], entry_sem.at[way, k])
        lax.fori_loop(start, start + fine, functools.partial(entry, way), 0, unroll=True)
        remote(xb_v.at[way, at], fin_v.at[way, core, at], send_sem.at[8], fin_sem.at[way, g], partner).start()

    main = 2 * N * 3 // 4
    share = (2 * N - main) // opts
    spans = (pl.ds(N, N), pl.ds(0, N))
    direct = (pl.ds(N, main - N), pl.ds(0, N))

    def quarter(who):
        return pl.ds(pl.multiple_of(main + who * share, share), share)

    def weight_pair(part, k, carry):
        lanes = pl.ds(pl.multiple_of(owner_after(k) * 2 * rblk, 2 * rblk), 2 * rblk)
        grads = dot_nn(gbt_b[spans[part], :], lay_v[:, lanes]).astype(BF16)
        wg_v[0, part, k] = grads[:, 0:rblk]
        wg_v[1, part, k] = grads[:, rblk:]
        return carry

    def chip_sum(part, k, carry):
        both = wg_v[core, part, k].astype(F32) + rd_v[part, k].astype(F32)
        rss_v[k, spans[part], :] = both.astype(BF16)
        return carry

    def sum_group(part, g):
        start = piece(g, fine)
        at = pl.ds(start, fine)
        wait_bytes(rd_v.at[part, at], rs_sem.at[part, g])
        lax.fori_loop(start, start + fine, functools.partial(chip_sum, part), 0, unroll=True)
        rows_at = direct[part]
        for k in reversed(range(max(1, start), start + fine)):
            remote(
                rss_v.at[k, rows_at], rsr_v.at[k, rows_at], send_sem.at[10], recv_sem.at[21 if part == 0 else 10], yz(k)[1]
            ).start()
        if part == 0 and (g + 1) * 2 % fines == 0:
            half_at = pl.ds(start, chips // 2)
            for k in range(1, opts):
                other, dev = xp(k)
                remote(
                    rss_v.at[half_at, quarter(other)], bx_v.at[opt, half_at], send_sem.at[18], recv_sem.at[18], dev
                ).start()

    def weight_group(part, g):
        start = piece(g, fine)
        at = pl.ds(start, fine)
        lax.fori_loop(start, start + fine, functools.partial(weight_pair, part), 0, unroll=True)
        remote(
            wg_v.at[1 - core, part, at], rd_v.at[part, at], send_sem.at[9], rs_sem.at[part, g], partner
        ).start()

    def arrived(part, sem):
        rows_at = direct[part]
        wait_bytes(rsr_v.at[pl.ds(0, chips - 1), rows_at], recv_sem.at[sem])
        acc = rsr_v[0, rows_at, :].astype(F32)
        for k in range(1, chips):
            acc = acc + rsr_v[k, rows_at, :].astype(F32)
        xg_v[opt, rows_at, :] = acc.astype(BF16)
        for k in range(1, opts):
            same(xg_v.at[opt, rows_at], send_sem.at[11], recv_sem.at[22 if part == 0 else 11], xp(k)[1]).start()

    for i in range(fines + behind):
        if i < fines:
            enter_group(0, i)
        if i >= behind:
            finish_group(0, i - behind)
    gbt_b[spans[0], :] = gbt_v[spans[0], :].astype(BF16)
    for i in range(fines + behind):
        for w in range(2 * i, min(2 * i + 2, fines)):
            weight_group(0, w)
        if i < fines:
            enter_group(1, i)
        for w in range(max(0, 2 * i - 4), min(2 * i - 2, fines)):
            sum_group(0, w)
        if i >= behind:
            finish_group(1, i - behind)
    rsr_v[0, direct[0], :] = rss_v[0, direct[0], :]
    bx_v[opt] = rss_v[:, quarter(opt)]
    gbt_b[spans[1], :] = gbt_v[spans[1], :].astype(BF16)
    for i in range(fines):
        weight_group(1, i)
        if i >= behind:
            sum_group(1, i - behind)
    wait_bytes(bx_v.at[pl.ds(0, opts - 1)], recv_sem.at[18])
    part_x = bx_v[0].astype(F32)
    for k in range(1, opts):
        part_x = part_x + bx_v[k].astype(F32)
    by_v[...] = part_x.astype(BF16)
    for k in far_first:
        remote(by_v.at[k], bz_v.at[k], send_sem.at[19], recv_sem.at[19], yz(k)[1]).start()
    bz_v[0] = by_v[0]
    for i in range(max(0, fines - behind), fines):
        sum_group(1, i)
    rsr_v[0, direct[1], :] = rss_v[0, direct[1], :]
    arrived(0, 21)

    lax.fori_loop(0, chips * 10 // 16, outer_pair, 0)
    wait_bytes(bz_v.at[pl.ds(0, chips - 1)], recv_sem.at[19])
    acc = bz_v[0].astype(F32)
    for k in range(1, chips):
        acc = acc + bz_v[k].astype(F32)
    bw_v[opt] = acc
    for k in range(1, opts):
        same(bw_v.at[opt], send_sem.at[20], recv_sem.at[20], xp(k)[1]).start()
    arrived(1, 10)
    lax.fori_loop(chips * 10 // 16, chips, outer_pair, 0)

    wait_bytes(mc_v.at[pl.ds(0, opts - 1)], recv_sem.at[14])
    for sem, rows_at in ((22, direct[0]), (11, direct[1])):
        wait_bytes(xg_v.at[pl.ds(0, opts - 1), rows_at], recv_sem.at[sem])
    acc = xg_v[0].astype(F32)
    for k in range(1, opts):
        acc = acc + xg_v[k].astype(F32)
    wait_bytes(bw_v.at[pl.ds(0, opts - 1)], recv_sem.at[20])
    grad = jnp.transpose(jnp.concatenate([acc] + [bw_v[k] for k in range(opts)], axis=0))
    gt_v[...] = grad

    def over_all(buf, row, base, combine_fn):
        buf[seq, 0:1] = row
        for k in range(1, seqs):
            same(buf.at[seq, 0:1], send_sem.at[base], recv_sem.at[base], ((seq + k) % seqs, opt)).start()
        wait_bytes(buf.at[pl.ds(0, seqs - 1), 0:1], recv_sem.at[base])
        value = buf[0, 0:1]
        for k in range(1, seqs):
            value = combine_fn(value, buf[k, 0:1])
        return value

    col_raw = over_all(s_v, jnp.sum(grad * grad, axis=0, keepdims=True), 16, jnp.add)
    raw_total = jnp.sum(col_raw, axis=1, keepdims=True)
    factor = jnp.minimum(1.0, clip_norm / jnp.sqrt(raw_total + norm_floor))

    def moment_of(code, part):
        return beta_one * code.astype(F32) * mscale_ref[...] + (1.0 - beta_one) * (part * factor)

    top = jnp.zeros((1, 2 * N), F32)
    for k in range(opts):
        part = moment_of(mc_v[k], gt_v[k * rows : (k + 1) * rows])
        top = jnp.maximum(top, jnp.max(jnp.abs(part), axis=0, keepdims=True))
    peak = over_all(m_v, top, 17, jnp.maximum)

    own = gt_v[pl.ds(pl.multiple_of(opt * rows, rows), rows), :]
    scaled = own * factor
    moment = moment_of(mc_v[opt], own)
    squares = scaled * scaled
    old_total = jnp.sum(dc_v[:, 1, 0:1], axis=0, keepdims=True)
    col_next = beta_two * colstat_ref[...] + (1.0 - beta_two) * (factor * factor * col_raw / dim + tiny_square)
    eye = lax.broadcasted_iota(jnp.int32, (rows, rows), 0) == lax.broadcasted_iota(jnp.int32, (rows, rows), 1)
    old_col = jnp.sum(jnp.where(eye, jnp.broadcast_to(old_row, (rows, rows)), 0.0), axis=1, keepdims=True)
    row_next = beta_two * old_col + (1.0 - beta_two) * (
        jnp.sum(squares, axis=1, keepdims=True) / (2 * N) + tiny_square
    )
    row_mean = (
        beta_two * old_total + (1.0 - beta_two) * (factor * factor * raw_total / (2 * N) + dim * tiny_square)
    ) / dim
    second = row_next * col_next / row_mean
    upd_ref[...] = moment / (jnp.sqrt(second) + adam_floor) + weight_decay * w_ref[...]
    scale_next = peak + peak_floor
    scaleo_ref[...] = scale_next
    codeo_ref[...] = (moment / scale_next).astype(BF16)
    colo_ref[...] = col_next
    rowo_ref[...] = jnp.sum(jnp.where(eye, jnp.broadcast_to(row_next, (rows, rows)), 0.0), axis=0, keepdims=True)

    wait_bytes(wl_v.at[0, 0, pl.ds(0, opts - 1)], send_sem.at[0])
    wait_bytes(dlo_v, send_sem.at[1])
    wait_bytes(wl_v.at[pl.ds(0, chips - 1), 0, :], send_sem.at[2])
    wait_bytes(wl_v, send_sem.at[3])
    wait_bytes(dc_v.at[pl.ds(0, chips - 1)], send_sem.at[4])
    wait_bytes(pt_v, send_sem.at[5])
    wait_bytes(cb_v.at[:, pl.ds(0, chips - 1)], send_sem.at[6])
    wait_bytes(ob_v.at[:, pl.ds(0, chips - 1)], send_sem.at[7])
    wait_bytes(xb_v, send_sem.at[8])
    wait_bytes(rd_v, send_sem.at[9])
    wait_bytes(rsr_v.at[pl.ds(0, chips - 1)], send_sem.at[10])
    wait_bytes(xg_v.at[pl.ds(0, opts - 1)], send_sem.at[11])
    wait_bytes(wr_v.at[pl.ds(0, chips - 1), 0, 0], send_sem.at[12])
    wait_bytes(rx_v.at[pl.ds(0, opts - 1)], send_sem.at[13])
    wait_bytes(mc_v.at[pl.ds(0, opts - 1)], send_sem.at[14])
    wait_bytes(wr_v.at[:, 0, pl.ds(0, opts - 1)], send_sem.at[15])
    wait_bytes(bx_v.at[pl.ds(0, opts - 1)], send_sem.at[18])
    wait_bytes(by_v.at[pl.ds(0, chips - 1)], send_sem.at[19])
    wait_bytes(bw_v.at[pl.ds(0, opts - 1)], send_sem.at[20])
    for base, buf in ((16, s_v), (17, m_v)):
        wait_bytes(buf.at[pl.ds(0, seqs - 1), 0:1], send_sem.at[base])


def copy_out(*refs):
    sem = refs[-1]
    copies = []
    gi_ref, gi_out = refs[0], refs[6]
    pieces = 4
    size = gi_ref.shape[0] // pieces
    for k in range(pieces):
        at = pl.ds(k * size, size)
        copies.append(pltpu.make_async_copy(gi_ref.at[at], gi_out.at[at], sem.at[k]))
    for k in range(1, 6):
        copies.append(pltpu.make_async_copy(refs[k], refs[6 + k], sem.at[pieces + k - 1]))
    for copy in copies:
        copy.start()
    for copy in copies:
        copy.wait()


def per_device(
    seqs, opts, layer_in, ssm_input, grad_out, log_decay, skip_gain, w_bc, m_code, m_scale, row_stat, col_stat
):
    heads = skip_gain.shape[0]
    tokens, width = ssm_input.shape[1:]
    dim = layer_in.shape[2]
    rows = w_bc.shape[0]
    chips = seqs // 2
    rblk = rows * opts
    vm = pl.BlockSpec(memory_space=pltpu.VMEM)
    hbm = pl.BlockSpec(memory_space=pl.ANY)
    state = (2, chips, N, N)
    main = 2 * N * 3 // 4
    share = (2 * N - main) // opts
    scratch = [
        pltpu.VMEM((tokens, width), BF16),
        pltpu.VMEM((tokens, width), BF16),
        pltpu.VMEM((tokens, dim), BF16),
        pltpu.VMEM((tokens, width), BF16),
        pltpu.VMEM((tokens, width), BF16),
        pltpu.VMEM((chips, 2, opts, rows, N), BF16),
        pltpu.VMEM((chips, 2, opts, rows, N), BF16),
        pltpu.VMEM((N, tokens), F32),
        pltpu.VMEM((1, heads), F32),
        pltpu.VMEM((rows, 2 * N), F32),
        pltpu.VMEM((1, 2 * N), F32),
        pltpu.VMEM((1, rows), F32),
        pltpu.VMEM((1, 2 * N), F32),
        pltpu.VMEM((2, N, BLOCK), F32),
        pltpu.VMEM((tokens, N), F32),
        pltpu.VMEM((2, 8, width), F32),
        pltpu.VMEM((2, BLOCK, BLOCK), F32),
        pltpu.VMEM((2, BLOCK, BLOCK), F32),
        pltpu.VMEM((tokens, 2 * N), F32),
        pltpu.VMEM((tokens, 2 * N), BF16),
        pltpu.VMEM((2 * N, tokens), BF16),
        pltpu.VMEM((N, width), F32),
        pltpu.VMEM((N, width), F32),
        pltpu.VMEM((2, 2, chips, N, N), BF16),
        pltpu.VMEM(state, BF16),
        pltpu.VMEM(state, BF16),
        pltpu.VMEM(state, BF16),
        pltpu.VMEM(state, BF16),
        pltpu.VMEM(state, BF16),
        pltpu.VMEM(state, BF16),
        pltpu.VMEM((2, 2, chips, N, N), BF16),
        pltpu.VMEM((2 * N, tokens), F32),
        pltpu.VMEM((2 * N, tokens), BF16),
        pltpu.VMEM((2, 2, chips, N, rblk), BF16),
        pltpu.VMEM((2, chips, N, rblk), BF16),
        pltpu.VMEM((chips, 2 * N, rblk), BF16),
        pltpu.VMEM((chips, main, rblk), BF16),
        pltpu.VMEM((opts, chips, share, rblk), BF16),
        pltpu.VMEM((chips, share, rblk), BF16),
        pltpu.VMEM((chips, share, rblk), BF16),
        pltpu.VMEM((opts, share, rblk), F32),
        pltpu.VMEM((opts, main, rblk), BF16),
        pltpu.VMEM((rblk, 2 * N), F32),
        pltpu.VMEM((opts, rows, 2 * N), BF16),
        pltpu.VMEM((opts, 8, N), F32),
        pltpu.VMEM((8, N), F32),
        pltpu.VMEM((8, N), F32),
        pltpu.VMEM((chips, 8, N), F32),
        pltpu.VMEM((seqs, 8, 2 * N), F32),
        pltpu.VMEM((seqs, 8, 2 * N), F32),
        pltpu.SemaphoreType.DMA((9,)),
        pltpu.SemaphoreType.DMA((7,)),
        pltpu.SemaphoreType.DMA((23,)),
        pltpu.SemaphoreType.DMA((23,)),
        pltpu.SemaphoreType.DMA((chips,)),
        pltpu.SemaphoreType.DMA((opts,)),
        pltpu.SemaphoreType.DMA((2, chips)),
        pltpu.SemaphoreType.DMA((2, 4)),
        pltpu.SemaphoreType.DMA((2, min(8, chips))),
        pltpu.SemaphoreType.DMA((2, min(8, chips))),
    ]
    shapes = (
        jax.ShapeDtypeStruct((tokens, width), BF16),
        jax.ShapeDtypeStruct((rows, 2 * N), F32),
        jax.ShapeDtypeStruct((rows, 2 * N), BF16),
        jax.ShapeDtypeStruct((1, 2 * N), F32),
        jax.ShapeDtypeStruct((1, rows), F32),
        jax.ShapeDtypeStruct((1, 2 * N), F32),
    )
    out = pl.pallas_call(
        functools.partial(kernel, seqs, opts),
        out_shape=tuple(pltpu.VMEM(a.shape, a.dtype) for a in shapes),
        in_specs=[hbm] * 10,
        out_specs=(vm, vm, vm, vm, vm, vm),
        scratch_shapes=scratch,
        compiler_params=pltpu.CompilerParams(
            collective_id=0, has_side_effects=True, vmem_limit_bytes=60_000_000
        ),
    )(
        ssm_input[0],
        grad_out[0],
        layer_in[0],
        log_decay[0],
        skip_gain.reshape(1, heads),
        w_bc,
        m_code,
        m_scale.reshape(1, 2 * N),
        row_stat.reshape(1, rows),
        col_stat.reshape(1, 2 * N),
    )
    grad_input, update, code_next, scale_next, row_next, col_next = pl.pallas_call(
        copy_out,
        out_shape=shapes,
        in_specs=[vm] * 6,
        out_specs=(hbm,) * 6,
        scratch_shapes=[pltpu.SemaphoreType.DMA((9,))],
        compiler_params=pltpu.CompilerParams(vmem_limit_bytes=4_000_000),
    )(*[pltpu.with_memory_space_constraint(a, pltpu.VMEM) for a in out])
    return (
        grad_input[None],
        update,
        code_next,
        scale_next.reshape(2 * N),
        row_next.reshape(rows),
        col_next.reshape(2 * N),
    )


def solution(mesh):
    both = ("seq", "opt")
    return jax.shard_map(
        functools.partial(per_device, mesh.shape["seq"], mesh.shape["opt"]),
        mesh=mesh,
        in_specs=(
            P("opt", "seq", None),
            P("opt", "seq", None),
            P("opt", "seq", None),
            P("opt", None, "seq"),
            P(),
            P(both, None),
            P(both, None),
            P(),
            P(both),
            P(),
        ),
        out_specs=(P("opt", "seq", None), P(both, None), P(both, None), P(), P(both), P()),
        check_vma=False,
    )
```

```python
import functools
import math

import jax
import jax.numpy as jnp
from jax import lax
from jax.experimental import pallas as pl
from jax.experimental.pallas import tpu as pltpu
from jax.sharding import PartitionSpec as P

MESH = pl.DeviceIdType.MESH
BLOCK = 256
N = 128
F32 = jnp.float32
BF16 = jnp.bfloat16
HIGH = lax.Precision.HIGHEST

beta_one = 0.9
beta_two = 0.95
weight_decay = 0.1
clip_norm = 1.0
tiny_square = 1e-30
adam_floor = 1e-08
peak_floor = 1e-06
norm_floor = 1e-06


def dot_nn(a, b, precision=None):
    return lax.dot_general(a, b, (((1,), (0,)), ((), ())), preferred_element_type=F32, precision=precision)


def dot_nt(a, b, precision=None):
    return lax.dot_general(a, b, (((1,), (1,)), ((), ())), preferred_element_type=F32, precision=precision)


def kernel(
    seqs,
    opts,
    x_hbm,
    dy_hbm,
    lay_hbm,
    logs_hbm,
    skip_hbm,
    w_hbm,
    code_hbm,
    mscale_hbm,
    rowstat_hbm,
    colstat_hbm,
    gi_v,
    upd_ref,
    codeo_ref,
    scaleo_ref,
    rowo_ref,
    colo_ref,
    x_v,
    dy_v,
    lay_v,
    xs_v,
    ds_v,
    wl_v,
    wr_v,
    logp_v,
    skip_ref,
    w_ref,
    mscale_ref,
    rowstat_ref,
    colstat_ref,
    r_v,
    rt_v,
    erow_v,
    mix_v,
    aff_v,
    proj_v,
    bc_v,
    bct_v,
    f0_v,
    k1_v,
    t_v,
    pt_v,
    cb_v,
    rb_v,
    ob_v,
    ib_v,
    xb_v,
    fin_v,
    gbt_v,
    gbt_b,
    wg_v,
    rd_v,
    rss_v,
    rsr_v,
    bx_v,
    by_v,
    bz_v,
    bw_v,
    xg_v,
    gt_v,
    mc_v,
    rx_v,
    dlo_v,
    dlp_v,
    dc_v,
    s_v,
    m_v,
    in_sem,
    small_sem,
    send_sem,
    recv_sem,
    blk_sem,
    half_sem,
    entry_sem,
    d2d_sem,
    fin_sem,
    rs_sem,
):
    heads = skip_ref.shape[1]
    chips = seqs // 2
    rows = w_ref.shape[0]
    rblk = rows * opts
    width = x_hbm.shape[1]
    dim = lay_hbm.shape[1]
    groups = 4
    lanes_g = width // groups
    fines = min(8, chips)
    fine = chips // fines
    parts = 4
    per = chips // parts

    seq = lax.axis_index("seq")
    opt = lax.axis_index("opt")
    chip = seq // 2
    core = seq % 2
    mate = chip * 2 + (1 - core)
    partner = (mate, opt)

    side = math.isqrt(chips)

    def step_of(i):
        return (i * (i + 1) // 2) % side

    def owner_after(e):
        zs = (chip // side + step_of(e // side)) % side
        ys = (chip % side + step_of(e % side)) % side
        return zs * side + ys

    def owner_before(e):
        zs = (chip // side + side - step_of(e // side)) % side
        ys = (chip % side + side - step_of(e % side)) % side
        return zs * side + ys

    def flip(i):
        return 2 * (i % 2) + i // 2 if side == 4 else i

    def opposite(e):
        return flip(e // side) * side + flip(e % side)

    far_first = tuple(range(chips - 1, 0, -1))

    def yz(e):
        other = owner_after(e)
        return other, (other * 2 + core, opt)

    def xp(k):
        other = (opt + k) % opts
        return other, (seq, other)

    def remote(src, dst, s_sem, r_sem, dev):
        return pltpu.make_async_remote_copy(
            src_ref=src, dst_ref=dst, send_sem=s_sem, recv_sem=r_sem, device_id=dev, device_id_type=MESH
        )

    def wait_bytes(ref, sem):
        pltpu.make_async_copy(ref, ref, sem).wait()

    def in_copies(g):
        lanes = pl.ds(g * lanes_g, lanes_g)
        return (
            pltpu.make_async_copy(x_hbm.at[:, lanes], x_v.at[:, lanes], in_sem.at[2 * g]),
            pltpu.make_async_copy(dy_hbm.at[:, lanes], dy_v.at[:, lanes], in_sem.at[2 * g + 1]),
        )

    lay_copy = pltpu.make_async_copy(lay_hbm, lay_v, in_sem.at[2 * groups])

    def small(source, target, k):
        return pltpu.make_async_copy(source, target, small_sem.at[k])

    smalls = [
        small(w_hbm, w_ref, 0),
        small(rowstat_hbm, rowstat_ref, 1),
        small(code_hbm, mc_v.at[opt], 2),
        small(logs_hbm, logp_v.at[pl.ds(0, heads)], 3),
        small(skip_hbm, skip_ref, 4),
        small(mscale_hbm, mscale_ref, 5),
        small(colstat_hbm, colstat_ref, 6),
    ]
    barrier = pltpu.get_barrier_semaphore()
    for k in reversed(range(1, chips)):
        for who in range(2):
            pl.semaphore_signal(barrier, inc=1, device_id=(owner_after(k) * 2 + who, opt), device_id_type=MESH)
    pl.semaphore_signal(barrier, inc=1, device_id=partner, device_id_type=MESH)
    for k in range(1, opts):
        pl.semaphore_signal(barrier, inc=1, device_id=xp(k)[1], device_id_type=MESH)
    for copy in smalls:
        copy.start()
    if heads < N:
        logp_v[heads:, :] = jnp.zeros((N - heads, logp_v.shape[1]), F32)
    for copy in smalls:
        copy.wait()
    for g in range(groups):
        for copy in in_copies(g):
            copy.start()
    lay_copy.start()

    wl_v[chip, core, opt] = w_ref[:, 0:N].astype(BF16)
    wr_v[chip, core, opt] = w_ref[:, N:].astype(BF16)
    old_row = rowstat_ref[...]
    rx_v[opt] = jnp.broadcast_to(jnp.sum(old_row, axis=1, keepdims=True), (8, N))


    def same(ref, s_sem, r_sem, dev):
        return remote(ref, ref, s_sem, r_sem, dev)

    pl.semaphore_wait(barrier, seqs - 1 + opts - 1)
    for k in range(1, opts):
        same(wl_v.at[chip, core, opt], send_sem.at[0], recv_sem.at[0], xp(k)[1]).start()
    for k in far_first:
        same(wr_v.at[chip, core, opt], send_sem.at[12], recv_sem.at[12], yz(k)[1]).start()
    for k in range(1, opts):
        same(rx_v.at[opt], send_sem.at[13], recv_sem.at[13], xp(k)[1]).start()
        same(mc_v.at[opt], send_sem.at[14], recv_sem.at[14], xp(k)[1]).start()

    row_i = lax.broadcasted_iota(jnp.int32, (BLOCK, BLOCK), 0)
    col_i = lax.broadcasted_iota(jnp.int32, (BLOCK, BLOCK), 1)
    upper = jnp.where(row_i <= col_i, 1.0, 0.0).astype(F32)
    lower = jnp.where(row_i >= col_i, 1.0, 0.0).astype(F32)
    for b in range(2):
        part = logp_v[:, b * BLOCK : (b + 1) * BLOCK]
        r_v[b] = dot_nn(part, upper, HIGH)
        rt_v[b * BLOCK : (b + 1) * BLOCK, :] = dot_nt(lower, part, HIGH)

    mix_v[...] = jnp.zeros_like(mix_v)
    lane_i = lax.broadcasted_iota(jnp.int32, (2 * BLOCK, N), 1)

    def column(h):
        return jnp.sum(jnp.where(lane_i == h, rt_v[...], 0.0), axis=1, keepdims=True)

    half = BLOCK // 2
    tri_a = lax.broadcasted_iota(jnp.int32, (half, BLOCK), 1) >= lax.broadcasted_iota(jnp.int32, (half, BLOCK), 0)
    tri_b = lax.broadcasted_iota(jnp.int32, (half, half), 1) >= lax.broadcasted_iota(jnp.int32, (half, half), 0)

    def decays(rt, rs):
        top = jnp.exp(jnp.where(tri_a, rs - rt[0:half], -jnp.inf))
        bottom = jnp.exp(jnp.where(tri_b, rs[:, half:] - rt[half:], -jnp.inf))
        return top, bottom

    def mix_pair(products, scales, hp, carry):
        adds = [[None, None], [None, None]]
        for j in range(2):
            h = hp * 2 + j
            lanes = pl.ds(pl.multiple_of(h * N, N), N)
            col = column(h)
            for b in range(2):
                at = pl.ds(b * BLOCK, BLOCK)
                xb = x_v[at, lanes]
                db = dy_v[at, lanes]
                rt = col[b * BLOCK : (b + 1) * BLOCK]
                if products:
                    prod = dot_nt(xb, db)
                    top, bottom = decays(rt, r_v[b, pl.ds(h, 1), :])
                    top = top * prod[0:half]
                    bottom = bottom * prod[half:, half:]
                    adds[b][0] = top if j == 0 else adds[b][0] + top
                    adds[b][1] = bottom if j == 0 else adds[b][1] + bottom
                if scales:
                    closing = rt[BLOCK - 1 : BLOCK]
                    erow_v[b, :, lanes] = jnp.broadcast_to(jnp.exp(closing), (8, N))
                    xs_v[at, lanes] = (xb.astype(F32) * jnp.exp(closing - rt)).astype(BF16)
                    ds_v[at, lanes] = (db.astype(F32) * jnp.exp(rt)).astype(BF16)
        if products:
            for b in range(2):
                mix_v[b, 0:half, :] += adds[b][0]
                mix_v[b, half:, half:] += adds[b][1]
        return carry

    pairs = heads // 2

    def mix_group(first_part, last_part, products=True):
        first_pair, last_pair = (pairs * part // 16 for part in (first_part, last_part))
        for g in range(groups):
            if first_pair <= g * (pairs // groups) < last_pair:
                for copy in in_copies(g):
                    copy.wait()
        lax.fori_loop(first_pair, last_pair, functools.partial(mix_pair, products, True), 0)

    def share_left(some):
        for k in some:
            block = wl_v.at[owner_before(k), core]
            wait_bytes(block, blk_sem.at[k])
            same(block, send_sem.at[3], recv_sem.at[3], partner).start()

    mix_group(0, 2)
    wait_bytes(wl_v.at[0, 0, pl.ds(0, opts - 1)], recv_sem.at[0])
    for k in far_first:
        same(wl_v.at[chip, core], send_sem.at[2], blk_sem.at[k], yz(k)[1]).start()
    same(wl_v.at[chip, core], send_sem.at[3], recv_sem.at[3], partner).start()
    wait_bytes(rx_v.at[pl.ds(0, opts - 1)], recv_sem.at[13])
    old_sum = rx_v[0]
    for k in range(1, opts):
        old_sum = old_sum + rx_v[k]
    dlo_v[...] = old_sum
    dlo_v[0:1, :] = rt_v[BLOCK - 1 : BLOCK, :] + rt_v[2 * BLOCK - 1 : 2 * BLOCK, :]
    remote(dlo_v, dlp_v, send_sem.at[1], recv_sem.at[1], partner).start()
    mix_group(2, 3)
    wait_bytes(wr_v.at[pl.ds(0, chips - 1), 0, 0], recv_sem.at[12])
    for k in range(1, opts):
        same(wr_v.at[:, core, opt], send_sem.at[15], half_sem.at[k], xp(k)[1]).start()
    same(wr_v.at[:, core, opt], send_sem.at[3], recv_sem.at[3], partner).start()
    mix_group(3, 5)
    wait_bytes(dlp_v, recv_sem.at[1])
    dc_v[chip] = dlo_v[...] + dlp_v[...]
    for k in far_first:
        same(dc_v.at[chip], send_sem.at[4], recv_sem.at[4], yz(k)[1]).start()
    mix_group(5, 9)
    share_left(far_first[: chips // 2])
    mix_group(9, 10)
    mix_group(10, 13, products=False)
    share_left(far_first[chips // 2 :])
    mix_group(13, 16, products=False)
    for k in range(1, opts):
        block = wr_v.at[:, core, (opt + opts - k) % opts]
        wait_bytes(block, half_sem.at[k])
        same(block, send_sem.at[3], recv_sem.at[3], partner).start()
    lay_copy.wait()

    def proj_half(who):
        rows_in = jnp.concatenate(
            [lay_v[:, pl.ds(pl.multiple_of((2 * o + who) * rblk, rblk), rblk)] for o in range(chips)], axis=1
        )
        weights = [ref[:, who].reshape(chips * rblk, N) for ref in (wl_v, wr_v)]
        return dot_nn(rows_in, jnp.concatenate(weights, axis=1))

    proj_v[...] = proj_half(core)
    wait_bytes(wl_v, recv_sem.at[3])
    proj = (proj_v[...] + proj_half(1 - core)).astype(BF16)
    bc_v[...] = proj
    bct_v[...] = jnp.transpose(proj.astype(F32)).astype(BF16)
    for b in range(2):
        at = slice(b * BLOCK, (b + 1) * BLOCK)
        aff_v[b] = dot_nt(bc_v[at, 0:N], bc_v[at, N : 2 * N])

    def add_pair(way, k, carry):
        lanes = pl.ds(pl.multiple_of(owner_after(k) * 2 * N, 2 * N), 2 * N)
        if way == 0:
            first_blk = dot_nn(bct_v[0:N, 0:BLOCK], xs_v[0:BLOCK, lanes])
            second_blk = dot_nn(bct_v[0:N, BLOCK:], xs_v[BLOCK:, lanes])
            f0_v[:, lanes] = first_blk
            both = (erow_v[1, 0:1, lanes] * first_blk + second_blk).astype(BF16)
        else:
            first_blk = dot_nn(bct_v[N:, 0:BLOCK], ds_v[0:BLOCK, lanes])
            second_blk = dot_nn(bct_v[N:, BLOCK:], ds_v[BLOCK:, lanes])
            k1_v[:, lanes] = second_blk
            both = (first_blk + erow_v[0, 0:1, lanes] * second_blk).astype(BF16)
        for j in range(2):
            t_v[way, j, k] = both[:, j * N : (j + 1) * N]
        return carry

    lane_r = lax.broadcasted_iota(jnp.int32, (1, N), 1)

    def decay_of(ref, h):
        return jnp.exp(jnp.sum(jnp.where(lane_r == h, ref[0:1, :], 0.0), axis=1, keepdims=True))

    first = core == 0

    def combine(way, k, carry):
        h = 2 * owner_after(k) + core
        mine = decay_of(dlo_v, h)
        theirs = decay_of(dlp_v, h)
        one = jnp.ones_like(mine)
        own = t_v[way, core, k].astype(F32)
        other = pt_v[way, k].astype(F32)
        if way == 0:
            both = jnp.where(first, theirs, one) * own + jnp.where(first, one, mine) * other
        else:
            both = jnp.where(first, one, theirs) * own + jnp.where(first, mine, one) * other
        cb_v[way, k] = both.astype(BF16)
        return carry

    def piece(g, size):
        return chips - (g + 1) * size

    def to_owner(way, k):
        sem = send_sem.at[6 if way == 0 else 21]
        return remote(cb_v.at[way, k], rb_v.at[way, chip], sem, recv_sem.at[6 + way], yz(k)[1])

    def combine_group(way, g):
        start = piece(g, per)
        at = pl.ds(start, per)
        wait_bytes(pt_v.at[way, at], d2d_sem.at[way, g])
        lax.fori_loop(start, start + per, functools.partial(combine, way), 0, unroll=True)
        if way == 0:
            for k in reversed(range(max(1, start), start + per)):
                to_owner(way, k).start()

    steps = [(way, g) for way in range(2) for g in range(parts)]
    for i, (way, g) in enumerate(steps):
        start = piece(g, per)
        at = pl.ds(start, per)
        lax.fori_loop(start, start + per, functools.partial(add_pair, way), 0, unroll=True)
        remote(t_v.at[way, 1 - core, at], pt_v.at[way, at], send_sem.at[5], d2d_sem.at[way, g], partner).start()
        if i >= 2:
            combine_group(*steps[i - 2])
    for i in range(len(steps) - 2, len(steps)):
        combine_group(*steps[i])
    for way in range(2):
        rb_v[way, chip] = cb_v[way, 0]

    lane_h = lax.broadcasted_iota(jnp.int32, (1, heads), 1)

    def inner_pair(hp, carry):
        for j in range(2):
            h = hp * 2 + j
            lanes = pl.ds(pl.multiple_of(h * N, N), N)
            col = column(h)
            gain = jnp.sum(jnp.where(lane_h == h, skip_ref[...], 0.0), axis=1, keepdims=True)
            for b in range(2):
                rt = col[b * BLOCK : (b + 1) * BLOCK]
                rs = r_v[b, pl.ds(h, 1), :]
                top, bottom = decays(rt, rs)
                top = (top * aff_v[b, 0:half, :]).astype(BF16)
                bottom = (bottom * aff_v[b, half:, half:]).astype(BF16)
                db = dy_v[pl.ds(b * BLOCK, BLOCK), lanes]
                low = db[half:]
                gi_v[pl.ds(b * BLOCK, half), lanes] = (dot_nn(top, db) + gain * db[0:half].astype(F32)).astype(BF16)
                gi_v[pl.ds(b * BLOCK + half, half), lanes] = (dot_nn(bottom, low) + gain * low.astype(F32)).astype(BF16)
        return carry

    lane_c = lax.broadcasted_iota(jnp.int32, (chips, N), 1)

    def scan_chips(way):
        wait_bytes(rb_v.at[way, pl.ds(0, chips - 1)], recv_sem.at[6 + way])
        chip_decay = jnp.exp(jnp.sum(jnp.where(lane_c == seq, dc_v[:, 0, :], 0.0), axis=1, keepdims=True))
        run = jnp.zeros((N, N), F32)
        for o in range(chips) if way == 0 else reversed(range(chips)):
            ob_v[way, o] = run.astype(BF16)
            run = chip_decay[o : o + 1] * run + rb_v[way, o].astype(F32)
        for k in far_first:
            other, dev = yz(k)
            remote(ob_v.at[way, other], ib_v.at[way, k], send_sem.at[7], entry_sem.at[way, k], dev).start()
        ib_v[way, 0] = ob_v[way, chip]

    lax.fori_loop(0, heads // 16, inner_pair, 0)
    wait_bytes(cb_v.at[0, pl.ds(0, chips - 1)], send_sem.at[6])
    for k in far_first:
        to_owner(1, k).start()
    lax.fori_loop(heads // 16, heads // 4, inner_pair, 0)
    lax.fori_loop(pairs * 10 // 16, pairs, functools.partial(mix_pair, True, False), 0)
    wait_bytes(dc_v.at[pl.ds(0, chips - 1)], recv_sem.at[4])
    scan_chips(0)
    lax.fori_loop(heads // 4, heads // 2, inner_pair, 0)
    scan_chips(1)

    for b in range(2):
        at = slice(b * BLOCK, (b + 1) * BLOCK)
        mix = mix_v[b].astype(BF16)
        gbt_v[0:N, at] = dot_nt(bct_v[N:, at], mix)
        gbt_v[N:, at] = dot_nn(bct_v[0:N, at], mix)

    def entry(way, k, carry):
        h = 2 * owner_before(k) + core
        back = opposite(k)
        mine = decay_of(dlo_v, h)
        theirs = decay_of(dlp_v, h)
        one = jnp.ones_like(mine)
        nil = jnp.zeros_like(mine)
        came = ib_v[way, k].astype(F32)
        own = t_v[way, core, back].astype(F32)
        other = pt_v[way, back].astype(F32)
        if way == 0:
            here = jnp.where(first, one, theirs) * came + jnp.where(first, nil, one) * other
            there = jnp.where(first, mine, one) * came + jnp.where(first, one, nil) * own
        else:
            here = jnp.where(first, theirs, one) * came + jnp.where(first, one, nil) * other
            there = jnp.where(first, one, mine) * came + jnp.where(first, nil, one) * own
        fin_v[way, core, k] = here.astype(BF16)
        xb_v[way, k] = there.astype(BF16)
        return carry

    def finish_pair(way, k, carry):
        o = owner_before(k)
        lanes = pl.ds(pl.multiple_of(o * 2 * N, 2 * N), 2 * N)
        came = jnp.concatenate([fin_v[way, 0, k], fin_v[way, 1, k]], axis=1)
        if way == 0:
            later = (f0_v[:, lanes] + erow_v[0, 0:1, lanes] * came.astype(F32)).astype(BF16)
            for b, st in enumerate((came, later)):
                at = slice(b * BLOCK, (b + 1) * BLOCK)
                gbt_v[N:, at] += dot_nt(st, ds_v[at, lanes])
            return carry
        earlier = (k1_v[:, lanes] + erow_v[1, 0:1, lanes] * came.astype(F32)).astype(BF16)
        for b, gr in enumerate((earlier, came)):
            at = slice(b * BLOCK, (b + 1) * BLOCK)
            gbt_v[0:N, at] += dot_nt(gr, xs_v[at, lanes])
        return carry

    def outer_pair(k, carry):
        o = owner_before(k)
        lanes = pl.ds(pl.multiple_of(o * 2 * N, 2 * N), 2 * N)
        came = jnp.concatenate([fin_v[1, 0, k], fin_v[1, 1, k]], axis=1)
        earlier = (k1_v[:, lanes] + erow_v[1, 0:1, lanes] * came.astype(F32)).astype(BF16)
        cols = [column(2 * o), column(2 * o + 1)]
        for b, gr in enumerate((earlier, came)):
            at = slice(b * BLOCK, (b + 1) * BLOCK)
            outer = dot_nn(bc_v[at, 0:N], gr)
            for j in range(2):
                sub = pl.ds(pl.multiple_of((o * 2 + j) * N, N), N)
                rt = cols[j][at]
                shrink = jnp.exp(rt[BLOCK - 1 : BLOCK] - rt)
                gi_v[at, sub] = (gi_v[at, sub].astype(F32) + shrink * outer[:, j * N : (j + 1) * N]).astype(BF16)
        return carry

    def finish_group(way, g):
        start = piece(g, fine)
        wait_bytes(xb_v.at[way, pl.ds(start, fine)], fin_sem.at[way, g])
        lax.fori_loop(start, start + fine, functools.partial(finish_pair, way), 0, unroll=True)

    behind = 3

    def enter_group(way, g):
        start = piece(g, fine)
        at = pl.ds(start, fine)
        for k in reversed(range(max(1, start), start + fine)):
            wait_bytes(ib_v.at[way, k], entry_sem.at[way, k])
        lax.fori_loop(start, start + fine, functools.partial(entry, way), 0, unroll=True)
        remote(xb_v.at[way, at], fin_v.at[way, core, at], send_sem.at[8], fin_sem.at[way, g], partner).start()

    main = 2 * N * 3 // 4
    share = (2 * N - main) // opts
    spans = (pl.ds(N, N), pl.ds(0, N))
    direct = (pl.ds(N, main - N), pl.ds(0, N))

    def quarter(who):
        return pl.ds(pl.multiple_of(main + who * share, share), share)

    def weight_pair(part, k, carry):
        lanes = pl.ds(pl.multiple_of(owner_after(k) * 2 * rblk, 2 * rblk), 2 * rblk)
        grads = dot_nn(gbt_b[spans[part], :], lay_v[:, lanes]).astype(BF16)
        wg_v[0, part, k] = grads[:, 0:rblk]
        wg_v[1, part, k] = grads[:, rblk:]
        return carry

    def chip_sum(part, k, carry):
        both = wg_v[core, part, k].astype(F32) + rd_v[part, k].astype(F32)
        rss_v[k, spans[part], :] = both.astype(BF16)
        return carry

    def sum_group(part, g):
        start = piece(g, fine)
        at = pl.ds(start, fine)
        wait_bytes(rd_v.at[part, at], rs_sem.at[part, g])
        lax.fori_loop(start, start + fine, functools.partial(chip_sum, part), 0, unroll=True)
        rows_at = direct[part]
        for k in reversed(range(max(1, start), start + fine)):
            remote(
                rss_v.at[k, rows_at], rsr_v.at[k, rows_at], send_sem.at[10], recv_sem.at[21 if part == 0 else 10], yz(k)[1]
            ).start()
        if part == 0 and (g + 1) * 2 % fines == 0:
            half_at = pl.ds(start, chips // 2)
            for k in range(1, opts):
                other, dev = xp(k)
                remote(
                    rss_v.at[half_at, quarter(other)], bx_v.at[opt, half_at], send_sem.at[18], recv_sem.at[18], dev
                ).start()

    def weight_group(part, g):
        start = piece(g, fine)
        at = pl.ds(start, fine)
        lax.fori_loop(start, start + fine, functools.partial(weight_pair, part), 0, unroll=True)
        remote(
            wg_v.at[1 - core, part, at], rd_v.at[part, at], send_sem.at[9], rs_sem.at[part, g], partner
        ).start()

    def arrived(part, sem):
        rows_at = direct[part]
        wait_bytes(rsr_v.at[pl.ds(0, chips - 1), rows_at], recv_sem.at[sem])
        acc = rsr_v[0, rows_at, :].astype(F32)
        for k in range(1, chips):
            acc = acc + rsr_v[k, rows_at, :].astype(F32)
        xg_v[opt, rows_at, :] = acc.astype(BF16)
        for k in range(1, opts):
            same(xg_v.at[opt, rows_at], send_sem.at[11], recv_sem.at[22 if part == 0 else 11], xp(k)[1]).start()

    for i in range(fines + behind):
        if i < fines:
            enter_group(0, i)
        if i >= behind:
            finish_group(0, i - behind)
    gbt_b[spans[0], :] = gbt_v[spans[0], :].astype(BF16)
    for i in range(fines + behind):
        for w in range(2 * i, min(2 * i + 2, fines)):
            weight_group(0, w)
        if i < fines:
            enter_group(1, i)
        for w in range(max(0, 2 * i - 4), min(2 * i - 2, fines)):
            sum_group(0, w)
        if i >= behind:
            finish_group(1, i - behind)
    rsr_v[0, direct[0], :] = rss_v[0, direct[0], :]
    bx_v[opt] = rss_v[:, quarter(opt)]
    gbt_b[spans[1], :] = gbt_v[spans[1], :].astype(BF16)
    for i in range(fines):
        weight_group(1, i)
        if i >= behind:
            sum_group(1, i - behind)
    wait_bytes(bx_v.at[pl.ds(0, opts - 1)], recv_sem.at[18])
    part_x = bx_v[0].astype(F32)
    for k in range(1, opts):
        part_x = part_x + bx_v[k].astype(F32)
    by_v[...] = part_x.astype(BF16)
    for k in far_first:
        remote(by_v.at[k], bz_v.at[k], send_sem.at[19], recv_sem.at[19], yz(k)[1]).start()
    bz_v[0] = by_v[0]
    for i in range(max(0, fines - behind), fines):
        sum_group(1, i)
    rsr_v[0, direct[1], :] = rss_v[0, direct[1], :]
    arrived(0, 21)

    lax.fori_loop(0, chips * 10 // 16, outer_pair, 0)
    wait_bytes(bz_v.at[pl.ds(0, chips - 1)], recv_sem.at[19])
    acc = bz_v[0].astype(F32)
    for k in range(1, chips):
        acc = acc + bz_v[k].astype(F32)
    bw_v[opt] = acc
    for k in range(1, opts):
        same(bw_v.at[opt], send_sem.at[20], recv_sem.at[20], xp(k)[1]).start()
    arrived(1, 10)
    lax.fori_loop(chips * 10 // 16, chips, outer_pair, 0)

    wait_bytes(mc_v.at[pl.ds(0, opts - 1)], recv_sem.at[14])
    for sem, rows_at in ((22, direct[0]), (11, direct[1])):
        wait_bytes(xg_v.at[pl.ds(0, opts - 1), rows_at], recv_sem.at[sem])
    acc = xg_v[0].astype(F32)
    for k in range(1, opts):
        acc = acc + xg_v[k].astype(F32)
    wait_bytes(bw_v.at[pl.ds(0, opts - 1)], recv_sem.at[20])
    grad = jnp.transpose(jnp.concatenate([acc] + [bw_v[k] for k in range(opts)], axis=0))
    gt_v[...] = grad

    def over_all(buf, row, base, combine_fn):
        buf[seq, 0:1] = row
        for e in far_first:
            there = owner_after(e) * 2
            for who in range(2):
                same(buf.at[seq, 0:1], send_sem.at[base], recv_sem.at[base], (there + who, opt)).start()
        same(buf.at[seq, 0:1], send_sem.at[base], recv_sem.at[base], partner).start()
        wait_bytes(buf.at[pl.ds(0, seqs - 1), 0:1], recv_sem.at[base])
        value = buf[0, 0:1]
        for k in range(1, seqs):
            value = combine_fn(value, buf[k, 0:1])
        return value

    col_raw = over_all(s_v, jnp.sum(grad * grad, axis=0, keepdims=True), 16, jnp.add)
    raw_total = jnp.sum(col_raw, axis=1, keepdims=True)
    factor = jnp.minimum(1.0, clip_norm / jnp.sqrt(raw_total + norm_floor))

    def moment_of(code, part):
        return beta_one * code.astype(F32) * mscale_ref[...] + (1.0 - beta_one) * (part * factor)

    top = jnp.zeros((1, 2 * N), F32)
    for k in range(opts):
        part = moment_of(mc_v[k], gt_v[k * rows : (k + 1) * rows])
        top = jnp.maximum(top, jnp.max(jnp.abs(part), axis=0, keepdims=True))
    peak = over_all(m_v, top, 17, jnp.maximum)

    own = gt_v[pl.ds(pl.multiple_of(opt * rows, rows), rows), :]
    scaled = own * factor
    moment = moment_of(mc_v[opt], own)
    squares = scaled * scaled
    old_total = jnp.sum(dc_v[:, 1, 0:1], axis=0, keepdims=True)
    col_next = beta_two * colstat_ref[...] + (1.0 - beta_two) * (factor * factor * col_raw / dim + tiny_square)
    eye = lax.broadcasted_iota(jnp.int32, (rows, rows), 0) == lax.broadcasted_iota(jnp.int32, (rows, rows), 1)
    old_col = jnp.sum(jnp.where(eye, jnp.broadcast_to(old_row, (rows, rows)), 0.0), axis=1, keepdims=True)
    row_next = beta_two * old_col + (1.0 - beta_two) * (
        jnp.sum(squares, axis=1, keepdims=True) / (2 * N) + tiny_square
    )
    row_mean = (
        beta_two * old_total + (1.0 - beta_two) * (factor * factor * raw_total / (2 * N) + dim * tiny_square)
    ) / dim
    second = row_next * col_next / row_mean
    upd_ref[...] = moment / (jnp.sqrt(second) + adam_floor) + weight_decay * w_ref[...]
    scale_next = peak + peak_floor
    scaleo_ref[...] = scale_next
    codeo_ref[...] = (moment / scale_next).astype(BF16)
    colo_ref[...] = col_next
    rowo_ref[...] = jnp.sum(jnp.where(eye, jnp.broadcast_to(row_next, (rows, rows)), 0.0), axis=0, keepdims=True)

    wait_bytes(wl_v.at[0, 0, pl.ds(0, opts - 1)], send_sem.at[0])
    wait_bytes(dlo_v, send_sem.at[1])
    wait_bytes(wl_v.at[pl.ds(0, chips - 1), 0, :], send_sem.at[2])
    wait_bytes(wl_v, send_sem.at[3])
    wait_bytes(dc_v.at[pl.ds(0, chips - 1)], send_sem.at[4])
    wait_bytes(pt_v, send_sem.at[5])
    wait_bytes(cb_v.at[1, pl.ds(0, chips - 1)], send_sem.at[21])
    wait_bytes(ob_v.at[:, pl.ds(0, chips - 1)], send_sem.at[7])
    wait_bytes(xb_v, send_sem.at[8])
    wait_bytes(rd_v, send_sem.at[9])
    wait_bytes(rsr_v.at[pl.ds(0, chips - 1)], send_sem.at[10])
    wait_bytes(xg_v.at[pl.ds(0, opts - 1)], send_sem.at[11])
    wait_bytes(wr_v.at[pl.ds(0, chips - 1), 0, 0], send_sem.at[12])
    wait_bytes(rx_v.at[pl.ds(0, opts - 1)], send_sem.at[13])
    wait_bytes(mc_v.at[pl.ds(0, opts - 1)], send_sem.at[14])
    wait_bytes(wr_v.at[:, 0, pl.ds(0, opts - 1)], send_sem.at[15])
    wait_bytes(bx_v.at[pl.ds(0, opts - 1)], send_sem.at[18])
    wait_bytes(by_v.at[pl.ds(0, chips - 1)], send_sem.at[19])
    wait_bytes(bw_v.at[pl.ds(0, opts - 1)], send_sem.at[20])
    for base, buf in ((16, s_v), (17, m_v)):
        wait_bytes(buf.at[pl.ds(0, seqs - 1), 0:1], send_sem.at[base])


def copy_out(*refs):
    sem = refs[-1]
    copies = []
    gi_ref, gi_out = refs[0], refs[6]
    pieces = 4
    size = gi_ref.shape[0] // pieces
    for k in range(pieces):
        at = pl.ds(k * size, size)
        copies.append(pltpu.make_async_copy(gi_ref.at[at], gi_out.at[at], sem.at[k]))
    for k in range(1, 6):
        copies.append(pltpu.make_async_copy(refs[k], refs[6 + k], sem.at[pieces + k - 1]))
    for copy in copies:
        copy.start()
    for copy in copies:
        copy.wait()


def per_device(
    seqs, opts, layer_in, ssm_input, grad_out, log_decay, skip_gain, w_bc, m_code, m_scale, row_stat, col_stat
):
    heads = skip_gain.shape[0]
    tokens, width = ssm_input.shape[1:]
    dim = layer_in.shape[2]
    rows = w_bc.shape[0]
    chips = seqs // 2
    rblk = rows * opts
    vm = pl.BlockSpec(memory_space=pltpu.VMEM)
    hbm = pl.BlockSpec(memory_space=pl.ANY)
    state = (2, chips, N, N)
    main = 2 * N * 3 // 4
    share = (2 * N - main) // opts
    scratch = [
        pltpu.VMEM((tokens, width), BF16),
        pltpu.VMEM((tokens, width), BF16),
        pltpu.VMEM((tokens, dim), BF16),
        pltpu.VMEM((tokens, width), BF16),
        pltpu.VMEM((tokens, width), BF16),
        pltpu.VMEM((chips, 2, opts, rows, N), BF16),
        pltpu.VMEM((chips, 2, opts, rows, N), BF16),
        pltpu.VMEM((N, tokens), F32),
        pltpu.VMEM((1, heads), F32),
        pltpu.VMEM((rows, 2 * N), F32),
        pltpu.VMEM((1, 2 * N), F32),
        pltpu.VMEM((1, rows), F32),
        pltpu.VMEM((1, 2 * N), F32),
        pltpu.VMEM((2, N, BLOCK), F32),
        pltpu.VMEM((tokens, N), F32),
        pltpu.VMEM((2, 8, width), F32),
        pltpu.VMEM((2, BLOCK, BLOCK), F32),
        pltpu.VMEM((2, BLOCK, BLOCK), F32),
        pltpu.VMEM((tokens, 2 * N), F32),
        pltpu.VMEM((tokens, 2 * N), BF16),
        pltpu.VMEM((2 * N, tokens), BF16),
        pltpu.VMEM((N, width), F32),
        pltpu.VMEM((N, width), F32),
        pltpu.VMEM((2, 2, chips, N, N), BF16),
        pltpu.VMEM(state, BF16),
        pltpu.VMEM(state, BF16),
        pltpu.VMEM(state, BF16),
        pltpu.VMEM(state, BF16),
        pltpu.VMEM(state, BF16),
        pltpu.VMEM(state, BF16),
        pltpu.VMEM((2, 2, chips, N, N), BF16),
        pltpu.VMEM((2 * N, tokens), F32),
        pltpu.VMEM((2 * N, tokens), BF16),
        pltpu.VMEM((2, 2, chips, N, rblk), BF16),
        pltpu.VMEM((2, chips, N, rblk), BF16),
        pltpu.VMEM((chips, 2 * N, rblk), BF16),
        pltpu.VMEM((chips, main, rblk), BF16),
        pltpu.VMEM((opts, chips, share, rblk), BF16),
        pltpu.VMEM((chips, share, rblk), BF16),
        pltpu.VMEM((chips, share, rblk), BF16),
        pltpu.VMEM((opts, share, rblk), F32),
        pltpu.VMEM((opts, main, rblk), BF16),
        pltpu.VMEM((rblk, 2 * N), F32),
        pltpu.VMEM((opts, rows, 2 * N), BF16),
        pltpu.VMEM((opts, 8, N), F32),
        pltpu.VMEM((8, N), F32),
        pltpu.VMEM((8, N), F32),
        pltpu.VMEM((chips, 8, N), F32),
        pltpu.VMEM((seqs, 8, 2 * N), F32),
        pltpu.VMEM((seqs, 8, 2 * N), F32),
        pltpu.SemaphoreType.DMA((9,)),
        pltpu.SemaphoreType.DMA((7,)),
        pltpu.SemaphoreType.DMA((23,)),
        pltpu.SemaphoreType.DMA((23,)),
        pltpu.SemaphoreType.DMA((chips,)),
        pltpu.SemaphoreType.DMA((opts,)),
        pltpu.SemaphoreType.DMA((2, chips)),
        pltpu.SemaphoreType.DMA((2, 4)),
        pltpu.SemaphoreType.DMA((2, min(8, chips))),
        pltpu.SemaphoreType.DMA((2, min(8, chips))),
    ]
    shapes = (
        jax.ShapeDtypeStruct((tokens, width), BF16),
        jax.ShapeDtypeStruct((rows, 2 * N), F32),
        jax.ShapeDtypeStruct((rows, 2 * N), BF16),
        jax.ShapeDtypeStruct((1, 2 * N), F32),
        jax.ShapeDtypeStruct((1, rows), F32),
        jax.ShapeDtypeStruct((1, 2 * N), F32),
    )
    out = pl.pallas_call(
        functools.partial(kernel, seqs, opts),
        out_shape=tuple(pltpu.VMEM(a.shape, a.dtype) for a in shapes),
        in_specs=[hbm] * 10,
        out_specs=(vm, vm, vm, vm, vm, vm),
        scratch_shapes=scratch,
        compiler_params=pltpu.CompilerParams(
            collective_id=0, has_side_effects=True, vmem_limit_bytes=60_000_000
        ),
    )(
        ssm_input[0],
        grad_out[0],
        layer_in[0],
        log_decay[0],
        skip_gain.reshape(1, heads),
        w_bc,
        m_code,
        m_scale.reshape(1, 2 * N),
        row_stat.reshape(1, rows),
        col_stat.reshape(1, 2 * N),
    )
    grad_input, update, code_next, scale_next, row_next, col_next = pl.pallas_call(
        copy_out,
        out_shape=shapes,
        in_specs=[vm] * 6,
        out_specs=(hbm,) * 6,
        scratch_shapes=[pltpu.SemaphoreType.DMA((9,))],
        compiler_params=pltpu.CompilerParams(vmem_limit_bytes=4_000_000),
    )(*[pltpu.with_memory_space_constraint(a, pltpu.VMEM) for a in out])
    return (
        grad_input[None],
        update,
        code_next,
        scale_next.reshape(2 * N),
        row_next.reshape(rows),
        col_next.reshape(2 * N),
    )


def solution(mesh):
    both = ("seq", "opt")
    return jax.shard_map(
        functools.partial(per_device, mesh.shape["seq"], mesh.shape["opt"]),
        mesh=mesh,
        in_specs=(
            P("opt", "seq", None),
            P("opt", "seq", None),
            P("opt", "seq", None),
            P("opt", None, "seq"),
            P(),
            P(both, None),
            P(both, None),
            P(),
            P(both),
            P(),
        ),
        out_specs=(P("opt", "seq", None), P(both, None), P(both, None), P(), P(both), P()),
        check_vma=False,
    )
```
